32 devices in a mesh: dp: 1 (over z), cp: 32 (over y, x, core).
Axes of the slice: x: 4, y: 4, z: 1, core: 2. Of those that a mesh axis runs over, the one named last changes fastest.
The devices are a block of a 4x4x8 slice.
Arguments:
- queries: bfloat16 [4, 4096, 8, 256], P('dp', 'cp')
- keys: bfloat16 [4, 4096, 1, 256], P('dp', 'cp')
- values: bfloat16 [4, 4096, 1, 256], P('dp', 'cp')
- out_grad: bfloat16 [4, 4096, 8, 256], P('dp', 'cp')
Outputs:
- output 1: bfloat16 [4, 4096, 8, 256], P('dp', 'cp')
- output 2: float32 [4, 8, 4096], P('dp', None, 'cp')
- output 3: bfloat16 [4, 4096, 8, 256], P('dp', 'cp')
- output 4: bfloat16 [4, 4096, 1, 256], P('dp', 'cp')
- output 5: bfloat16 [4, 4096, 1, 256], P('dp', 'cp')
All inputs are finite; a program needn't handle non-finite values.
Results may differ from the reference program's by a relative error of at most 0.0191514.
Values are sent between devices in bfloat16 or wider.
A program may use at most 768 MiB of HBM per device.

```python
import jax
import jax.numpy as jnp
from jax import lax

BATCH = 4
SEQ = 4096
HEADS = 8
KV_HEADS = 1
HEAD = 256
QBLOCK = 128

RATIO = HEADS // KV_HEADS
SCALE = HEAD ** -0.5
NUM_BLOCKS = SEQ // QBLOCK


def setup_inputs(seed: int = 0, part: int = 0) -> dict:
    base_key = jax.random.fold_in(jax.random.key(seed), part)
    rng_keys = jax.random.split(base_key, 4)
    q_shape = (BATCH, SEQ, HEADS, HEAD)
    kv_shape = (BATCH, SEQ, KV_HEADS, HEAD)
    queries = jax.random.normal(rng_keys[0], q_shape, jnp.float32).astype(jnp.bfloat16)
    keys = jax.random.normal(rng_keys[1], kv_shape, jnp.float32).astype(jnp.bfloat16)
    values = jax.random.normal(rng_keys[2], kv_shape, jnp.float32).astype(jnp.bfloat16)
    out_grad = jax.random.normal(rng_keys[3], q_shape, jnp.float32).astype(jnp.bfloat16)
    return {"queries": queries, "keys": keys, "values": values, "out_grad": out_grad}


def reference(queries, keys, values, out_grad):
    keys_f = keys.astype(jnp.float32)
    values_f = values.astype(jnp.float32)
    key_pos = jnp.arange(SEQ)
    query_blocks = jnp.moveaxis(queries.reshape(BATCH, NUM_BLOCKS, QBLOCK, KV_HEADS, RATIO, HEAD), 1, 0)
    grad_blocks = jnp.moveaxis(out_grad.reshape(BATCH, NUM_BLOCKS, QBLOCK, KV_HEADS, RATIO, HEAD), 1, 0)

    def block_step(carry, block_in):
        grad_key, grad_value = carry
        block_idx, query_blk, grad_blk = block_in
        query_f = query_blk.astype(jnp.float32)
        grad_f = grad_blk.astype(jnp.float32)
        query_pos = block_idx * QBLOCK + jnp.arange(QBLOCK)
        causal = query_pos[:, None] >= key_pos[None, :]
        scores = jnp.einsum("bqgrd,bkgd->bgrqk", query_f, keys_f) * SCALE
        scores = jnp.where(causal, scores, -jnp.inf)
        row_max = jnp.max(scores, axis=-1, keepdims=True)
        row_lse = row_max + jnp.log(jnp.sum(jnp.exp(scores - row_max), axis=-1, keepdims=True))
        prob_mat = jnp.exp(scores - row_lse)
        prob_round = prob_mat.astype(jnp.bfloat16).astype(jnp.float32)
        out_blk = jnp.einsum("bgrqk,bkgd->bqgrd", prob_round, values_f).astype(jnp.bfloat16)
        delta = jnp.einsum("bqgrd,bqgrd->bgrq", grad_f, out_blk.astype(jnp.float32))
        grad_prob = jnp.einsum("bqgrd,bkgd->bgrqk", grad_f, values_f)
        grad_score = prob_mat * (grad_prob - delta[..., None])
        score_round = grad_score.astype(jnp.bfloat16).astype(jnp.float32)
        grad_query = jnp.einsum("bgrqk,bkgd->bqgrd", score_round, keys_f) * SCALE
        grad_key = grad_key + jnp.einsum("bgrqk,bqgrd->bkgd", score_round, query_f) * SCALE
        grad_value = grad_value + jnp.einsum("bgrqk,bqgrd->bkgd", prob_round, grad_f)
        return (grad_key, grad_value), (out_blk, row_lse[..., 0], grad_query.astype(jnp.bfloat16))

    zero_kv = jnp.zeros((BATCH, SEQ, KV_HEADS, HEAD), jnp.float32)
    carry_out, block_outs = lax.scan(block_step, (zero_kv, zero_kv), (jnp.arange(NUM_BLOCKS), query_blocks, grad_blocks))
    out_blocks, lse_blocks, dq_blocks = block_outs
    attn_out = jnp.moveaxis(out_blocks, 0, 1).reshape(BATCH, SEQ, HEADS, HEAD)
    row_lse = jnp.moveaxis(lse_blocks, 0, 3).reshape(BATCH, HEADS, SEQ)
    grad_query = jnp.moveaxis(dq_blocks, 0, 1).reshape(BATCH, SEQ, HEADS, HEAD)
    grad_key = carry_out[0].astype(jnp.bfloat16)
    grad_value = carry_out[1].astype(jnp.bfloat16)
    return attn_out, row_lse, grad_query, grad_key, grad_value
```

```python
import functools
import math

import jax
import jax.numpy as jnp
from jax import lax
from jax.experimental import pallas as pl
from jax.experimental.pallas import tpu as pltpu
from jax.sharding import PartitionSpec as P

F32 = jnp.float32
BF16 = jnp.bfloat16
LN2 = math.log(2.0)


def dot(lhs, rhs):
    return jnp.dot(lhs, rhs, preferred_element_type=F32)


def attention_kernel(q_in, do_in, k_in, v_in, out, lse_out, dq_out, dk_out, dv_out,
                     qs, dos, qt, dot_t, kv, ot, ot_low, o_st, m_s, l_s, lse2, delta, lse_st, p_s, ds_s,
                     dqt, dq_st, dkdv, sib, peer, fin,
                     loc_sem, kv1_s, kv1_r, kv2_s, kvd_s, kv_r, q_sem, do_sem, o_sem, ls_sem, dq_sem,
                     r1_s, r1_r, r2_s, r2_r, r3_s, r3_r):
    tokens, head_dim = k_in.shape[1], k_in.shape[2]
    rows = q_in.shape[1]
    heads = rows // tokens
    blocks = kv.shape[1]
    chunks = blocks // 2
    keys = 2 * tokens
    side = 4
    scale = head_dim ** -0.5
    alpha = scale / LN2
    tile = min(256, rows)

    me = lax.axis_index("cp")
    core = me % 2
    chip = me // 2
    x, y = chip % side, chip // side
    qx, qy = x // 2, y // 2
    ux, uy = x + qx * (3 - 2 * x), y + qy * (3 - 2 * y)
    batch = 2 * qy + qx
    sibling = me + 1 - 2 * core

    def flip(f):
        fx, fy = f % 2, f // 2
        return ((y + fy * (3 - 2 * y)) * side + x + fx * (3 - 2 * x)) * 2 + core

    def flip_batch(f):
        fx, fy = f % 2, f // 2
        return 2 * (qy + fy * (1 - 2 * qy)) + qx + fx * (1 - 2 * qx)

    def group(a):
        ax, ay = a % 2, a // 2
        return ((y + ay * (1 + 4 * qy - 2 * y)) * side + x + ax * (1 + 4 * qx - 2 * x)) * 2 + core

    def remote(src, dst, send, recv, device):
        return pltpu.make_async_remote_copy(
            src_ref=src, dst_ref=dst, send_sem=send, recv_sem=recv,
            device_id={"cp": device}, device_id_type=pl.DeviceIdType.MESH)

    barrier = pltpu.get_barrier_semaphore()
    for device in [flip(f) for f in (1, 2, 3)] + [group(a) for a in (1, 2, 3)] + [sibling]:
        pl.semaphore_signal(barrier, inc=1, device_id={"cp": device}, device_id_type=pl.DeviceIdType.MESH)
    pl.semaphore_wait(barrier, 7)

    own = [
        pltpu.make_async_copy(k_in.at[batch], kv.at[0, me], loc_sem.at[0]),
        pltpu.make_async_copy(v_in.at[batch], kv.at[1, me], loc_sem.at[1]),
        pltpu.make_async_copy(q_in.at[batch], qs.at[0], loc_sem.at[2]),
        pltpu.make_async_copy(do_in.at[batch], dos.at[0], loc_sem.at[3]),
    ]
    for copy in own:
        copy.start()

    def kv1(f, which):
        src = (k_in, v_in)[which]
        return remote(src.at[flip_batch(f)], kv.at[which, me], kv1_s.at[which, f - 1], kv1_r.at[which, f - 1], flip(f))

    def q_copy(f):
        return remote(q_in.at[flip_batch(f)], qs.at[f], q_sem.at[0, f - 1], q_sem.at[1, f - 1], flip(f))

    def do_copy(f):
        return remote(do_in.at[flip_batch(f)], dos.at[f], do_sem.at[0, f - 1], do_sem.at[1, f - 1], flip(f))

    for f in (1, 2, 3):
        kv1(f, 0).start()
        kv1(f, 1).start()
    for f in (1, 2, 3):
        q_copy(f).start()
    for f in (1, 2, 3):
        do_copy(f).start()

    def kv2(a, f):
        g = flip(f)
        return remote(kv.at[:, g], kv.at[:, g], kv2_s.at[(a - 1) * 4 + f], kv_r.at[g], group(a))

    def kvd(g):
        return remote(kv.at[:, g], kv.at[:, g], kvd_s.at[g // 2], kv_r.at[g], sibling)

    own[0].wait()
    own[1].wait()
    for f in range(4):
        if f:
            kv1(f, 0).wait_recv()
            kv1(f, 1).wait_recv()
        for a in (1, 2, 3):
            kv2(a, f).start()
        kvd(flip(f)).start()

    def member(a, f):
        ax, ay, fx, fy = a % 2, a // 2, f % 2, f // 2
        xa = x + ax * (1 + 4 * qx - 2 * x)
        ya = y + ay * (1 + 4 * qy - 2 * y)
        return ((ya + fy * (3 - 2 * ya)) * side + xa + fx * (3 - 2 * xa)) * 2 + core

    def arrive(i, carry):
        g = member(1 + i % 3, i // 3)
        remote(kv.at[:, g], kv.at[:, g], kvd_s.at[g // 2], kv_r.at[g], sibling).wait_recv()
        kvd(g).start()
        return carry

    lax.fori_loop(0, 12, arrive, 0)

    def arrive_sibling(i, carry):
        g = 2 * i + 1 - core
        remote(kv.at[:, g], kv.at[:, g], kvd_s.at[i], kv_r.at[g], sibling).wait_recv()
        return carry

    lax.fori_loop(0, chunks, arrive_sibling, 0)

    def transpose_rows(src, dst, f):
        for r in range(rows // tile):
            dst[f, :, r * tile:(r + 1) * tile] = src[f, r * tile:(r + 1) * tile, :].T

    def visible(r):
        key = lax.broadcasted_iota(jnp.int32, (keys, tile), 0) - core * tokens
        token = (lax.broadcasted_iota(jnp.int32, (keys, tile), 1) + r * tile) // heads
        return key <= token

    def load_chunk(which, j):
        return kv[which, pl.ds(2 * j, 2)].reshape(keys, head_dim)

    def forward(f, j, masked):
        k_blk = load_chunk(0, j)
        vt_blk = load_chunk(1, j).T
        for r in range(rows // tile):
            cols = slice(r * tile, (r + 1) * tile)
            s = dot(k_blk, qt[f, :, cols]) * alpha
            if masked:
                s = jnp.where(visible(r), s, -jnp.inf)
            m_old = m_s[:, cols]
            m_new = jnp.maximum(m_old, jnp.max(s, axis=0, keepdims=True))
            p = jnp.exp2(s - m_new)
            corr = jnp.exp2(m_old - m_new)
            l_s[:, cols] = l_s[:, cols] * corr + jnp.sum(p, axis=0, keepdims=True)
            m_s[:, cols] = m_new
            ot[:, cols] = ot[:, cols] * corr + dot(vt_blk, p.astype(BF16))

    def o_copy(f):
        return remote(o_st.at[f], out.at[batch], o_sem.at[0, f - 1], o_sem.at[1, f - 1], flip(f))

    def lse_copy(f):
        return remote(lse_st.at[f], lse_out.at[batch], ls_sem.at[0, f - 1], ls_sem.at[1, f - 1], flip(f))

    own_out = [
        pltpu.make_async_copy(o_st.at[0], out.at[batch], loc_sem.at[4]),
        pltpu.make_async_copy(lse_st.at[0], lse_out.at[batch], loc_sem.at[5]),
        pltpu.make_async_copy(dq_st.at[0], dq_out.at[batch], loc_sem.at[6]),
        pltpu.make_async_copy(fin.at[0, 0], dk_out.at[batch], loc_sem.at[7]),
        pltpu.make_async_copy(fin.at[0, 1], dv_out.at[batch], loc_sem.at[8]),
    ]

    def forward_slot(f):
        transpose_rows(qs, qt, f)
        m_s[...] = jnp.full(m_s.shape, -jnp.inf, F32)
        l_s[...] = jnp.zeros(l_s.shape, F32)
        ot[...] = jnp.zeros(ot.shape, F32)
        last = flip(f) // 2

        def body(j, carry):
            forward(f, j, False)
            return carry

        lax.fori_loop(0, last, body, 0)
        forward(f, last, True)
        lse = m_s[...] + jnp.log2(l_s[...])
        lse2[f] = lse
        lse_st[f] = lse * LN2
        for r in range(rows // tile):
            cols = slice(r * tile, (r + 1) * tile)
            low = (ot[:, cols] * (1.0 / l_s[:, cols])).astype(BF16)
            ot_low[f, :, cols] = low
            o_st[f, cols, :] = low.T

    own[2].wait()
    forward_slot(0)
    own_out[0].start()
    own_out[1].start()

    def forward_rest(f, carry):
        q_copy(f).wait_recv()
        forward_slot(f)
        o_copy(f).start()
        lse_copy(f).start()
        return carry

    lax.fori_loop(1, 4, forward_rest, 0)

    def prepare(f):
        transpose_rows(dos, dot_t, f)
        for r in range(rows // tile):
            cols = slice(r * tile, (r + 1) * tile)
            prod = ot_low[f, :, cols].astype(F32) * dot_t[f, :, cols].astype(F32)
            delta[f, :, cols] = jnp.sum(prod, axis=0, keepdims=True)
        dqt[f] = jnp.zeros(dqt.shape[1:], F32)

    own[3].wait()
    prepare(0)

    def prepare_rest(f, carry):
        do_copy(f).wait_recv()
        prepare(f)
        return carry

    lax.fori_loop(1, 4, prepare_rest, 0)

    def backward(f, j, masked):
        k_blk = load_chunk(0, j)
        v_blk = load_chunk(1, j)
        kt_blk = k_blk.T
        for r in range(rows // tile):
            cols = slice(r * tile, (r + 1) * tile)
            s = dot(k_blk, qt[f, :, cols]) * alpha
            p = jnp.exp2(s - lse2[f, :, cols])
            if masked:
                p = jnp.where(visible(r), p, 0.0)
            dp = dot(v_blk, dot_t[f, :, cols])
            ds = p * (dp - delta[f, :, cols])
            p_s[:, cols] = p.astype(BF16)
            ds_s[:, cols] = ds.astype(BF16)
        shape = (2, tokens, head_dim)
        dkdv[1, pl.ds(2 * j, 2)] += dot(p_s[...], dos[f]).reshape(shape)
        dkdv[0, pl.ds(2 * j, 2)] += dot(ds_s[...], qs[f]).reshape(shape)
        for r in range(rows // tile):
            cols = slice(r * tile, (r + 1) * tile)
            dqt[f, :, cols] += dot(kt_blk, ds_s[:, cols])

    def dq_copy(f):
        return remote(dq_st.at[f], dq_out.at[batch], dq_sem.at[0, f - 1], dq_sem.at[1, f - 1], flip(f))

    def finish_dq(f):
        for r in range(rows // tile):
            cols = slice(r * tile, (r + 1) * tile)
            dq_st[f, cols, :] = (dqt[f, :, cols] * scale).astype(BF16).T

        @pl.when(f == 0)
        def _():
            own_out[2].start()

        @pl.when(f > 0)
        def _():
            dq_copy(f).start()

    def r1(j):
        return remote(dkdv.at[:, 2 * j + 1 - core], sib.at[:, j], r1_s.at[j], r1_r.at[j], sibling)

    def r2(g, a, f):
        i = (a - 1) * 4 + f
        return remote(dkdv.at[:, g], peer.at[i], r2_s.at[i], r2_r.at[i], group(a))

    def reduce_chunk(j):
        g = 2 * j + core
        r1(j).wait_recv()
        dkdv[:, g] += sib[:, j]
        xb, yb = j % side, j // side
        bx, by = xb // 2, yb // 2
        vx, vy = xb + bx * (3 - 2 * xb), yb + by * (3 - 2 * yb)
        a = (ux + vx - 2 * ux * vx) + 2 * (uy + vy - 2 * uy * vy)
        f = (qx + bx - 2 * qx * bx) + 2 * (qy + by - 2 * qy * by)

        @pl.when(a > 0)
        def _():
            r2(g, a, f).start()

    def backward_chunk(j, carry):
        dkdv[:, pl.ds(2 * j, 2)] = jnp.zeros((2, 2, tokens, head_dim), F32)

        def slot(f, inner):
            last = flip(f) // 2

            @pl.when(j < last)
            def _():
                backward(f, j, False)

            @pl.when(j == last)
            def _():
                backward(f, j, True)
                finish_dq(f)

            return inner

        lax.fori_loop(0, 4, slot, 0)
        r1(j).start()

        @pl.when(j > 0)
        def _():
            reduce_chunk(j - 1)

        return carry

    lax.fori_loop(0, chunks, backward_chunk, 0)
    reduce_chunk(chunks - 1)

    def fin_copy(f, which):
        dst = (dk_out, dv_out)[which]
        return remote(fin.at[f, which], dst.at[batch], r3_s.at[which, f - 1], r3_r.at[which, f - 1], flip(f))

    def finish_kv(f):
        g = flip(f)
        for a in (1, 2, 3):
            r2(g, a, f).wait_recv()
        total = dkdv[:, g] + peer[f] + peer[4 + f] + peer[8 + f]
        fin[f, 0] = (total[0] * scale).astype(BF16)
        fin[f, 1] = total[1].astype(BF16)

    for f in (1, 2, 3, 0):
        finish_kv(f)
        if f:
            fin_copy(f, 0).start()
            fin_copy(f, 1).start()
        else:
            own_out[3].start()
            own_out[4].start()

    for f in (1, 2, 3):
        for which in (0, 1):
            kv1(f, which).wait_send()
            fin_copy(f, which).wait()
        q_copy(f).wait_send()
        do_copy(f).wait_send()
        o_copy(f).wait()
        lse_copy(f).wait()
        dq_copy(f).wait()
    for copy in own_out:
        copy.wait()

    def drain(i, carry):
        kv2(1 + i // 4, i % 4).wait_send()
        r2(flip(i % 4), 1 + i // 4, i % 4).wait_send()
        return carry

    lax.fori_loop(0, 12, drain, 0)

    def drain_sibling(j, carry):
        kvd(2 * j + core).wait_send()
        r1(j).wait_send()
        return carry

    lax.fori_loop(0, chunks, drain_sibling, 0)


def solution(mesh):
    cp_size = mesh.shape["cp"]

    def attention_shard(queries, keys, values, out_grad):
        batch, tokens, heads, head_dim = queries.shape
        rows = tokens * heads
        q_rows = queries.reshape(batch, rows, head_dim)
        do_rows = out_grad.reshape(batch, rows, head_dim)
        k_rows = keys.reshape(batch, tokens, head_dim)
        v_rows = values.reshape(batch, tokens, head_dim)
        any_spec = pl.BlockSpec(memory_space=pl.ANY)
        dma = pltpu.SemaphoreType.DMA
        block = (tokens, head_dim)
        shapes = [
            jax.ShapeDtypeStruct((batch, rows, head_dim), BF16),
            jax.ShapeDtypeStruct((batch, 1, rows), F32),
            jax.ShapeDtypeStruct((batch, rows, head_dim), BF16),
            jax.ShapeDtypeStruct((batch,) + block, BF16),
            jax.ShapeDtypeStruct((batch,) + block, BF16),
        ]
        scratch = [
            pltpu.VMEM((4, rows, head_dim), BF16),
            pltpu.VMEM((4, rows, head_dim), BF16),
            pltpu.VMEM((4, head_dim, rows), BF16),
            pltpu.VMEM((4, head_dim, rows), BF16),
            pltpu.VMEM((2, cp_size) + block, BF16),
            pltpu.VMEM((head_dim, rows), F32),
            pltpu.VMEM((4, head_dim, rows), BF16),
            pltpu.VMEM((4, rows, head_dim), BF16),
            pltpu.VMEM((1, rows), F32),
            pltpu.VMEM((1, rows), F32),
            pltpu.VMEM((4, 1, rows), F32),
            pltpu.VMEM((4, 1, rows), F32),
            pltpu.VMEM((4, 1, rows), F32),
            pltpu.VMEM((2 * tokens, rows), BF16),
            pltpu.VMEM((2 * tokens, rows), BF16),
            pltpu.VMEM((4, head_dim, rows), F32),
            pltpu.VMEM((4, rows, head_dim), BF16),
            pltpu.VMEM((2, cp_size) + block, F32),
            pltpu.VMEM((2, cp_size // 2) + block, F32),
            pltpu.VMEM((12, 2) + block, F32),
            pltpu.VMEM((4, 2) + block, BF16),
            dma((9,)), dma((2, 3)), dma((2, 3)), dma((12,)), dma((cp_size // 2,)), dma((cp_size,)),
            dma((2, 3)), dma((2, 3)), dma((2, 3)), dma((2, 3)), dma((2, 3)),
            dma((cp_size // 2,)), dma((cp_size // 2,)), dma((12,)), dma((12,)), dma((2, 3)), dma((2, 3)),
        ]
        out, lse, dq, dk, dv = pl.pallas_call(
            attention_kernel,
            out_shape=shapes,
            in_specs=[any_spec] * 4,
            out_specs=[any_spec] * 5,
            scratch_shapes=scratch,
            name="attention",
            compiler_params=pltpu.CompilerParams(
                collective_id=0, has_side_effects=True, vmem_limit_bytes=60 * 1024 * 1024),
        )(q_rows, do_rows, k_rows, v_rows)
        row_lse = jnp.transpose(lse.reshape(batch, tokens, heads), (0, 2, 1))
        return out.reshape(queries.shape), row_lse, dq.reshape(queries.shape), dk.reshape(keys.shape), dv.reshape(values.shape)

    seq_spec = P("dp", "cp")
    return jax.shard_map(attention_shard, mesh=mesh, in_specs=(seq_spec, seq_spec, seq_spec, seq_spec), out_specs=(seq_spec, P("dp", None, "cp"), seq_spec, seq_spec, seq_spec), check_vma=False)
```

```python
import functools
import math

import jax
import jax.numpy as jnp
from jax import lax
from jax.experimental import pallas as pl
from jax.experimental.pallas import tpu as pltpu
from jax.sharding import PartitionSpec as P

F32 = jnp.float32
BF16 = jnp.bfloat16
LN2 = math.log(2.0)


def dot(lhs, rhs):
    return jnp.dot(lhs, rhs, preferred_element_type=F32)


def attention_kernel(q_in, do_in, k_in, v_in, out, lse_out, dq_out, dk_out, dv_out,
                     qs, dos, qt, dot_t, kv, ot, ot_low, o_st, m_s, l_s, lse2, delta, lse_st, bias, s_s, top_s, p_s, ds_s,
                     dqt, dq_st, dkdv, sib, peer, relay, fin,
                     loc_sem, kv1_s, kv1_r, kv2_s, kvf_s, kvd_s, kv_r, q_sem, do_sem, o_sem, ls_sem, dq_sem,
                     r1_s, r1_r, r2_s, r2_r, rl_s, rl_r, r3_s, r3_r, gate):
    tokens, head_dim = k_in.shape[1], k_in.shape[2]
    rows = q_in.shape[1]
    heads = rows // tokens
    blocks = kv.shape[1]
    chunks = blocks // 2
    keys = 2 * tokens
    side = 4
    scale = head_dim ** -0.5
    alpha = scale / LN2
    tile = min(256, rows)

    me = lax.axis_index("cp")
    core = me % 2
    chip = me // 2
    x, y = chip % side, chip // side
    qx, qy = x // 2, y // 2
    ux, uy = x + qx * (3 - 2 * x), y + qy * (3 - 2 * y)
    batch = 2 * qy + qx
    sibling = me + 1 - 2 * core

    def flip(f):
        fx, fy = f % 2, f // 2
        return ((y + fy * (3 - 2 * y)) * side + x + fx * (3 - 2 * x)) * 2 + core

    def flip_batch(f):
        fx, fy = f % 2, f // 2
        return 2 * (qy + fy * (1 - 2 * qy)) + qx + fx * (1 - 2 * qx)

    def group(a):
        ax, ay = a % 2, a // 2
        return ((y + ay * (1 + 4 * qy - 2 * y)) * side + x + ax * (1 + 4 * qx - 2 * x)) * 2 + core

    def remote(src, dst, send, recv, device):
        return pltpu.make_async_remote_copy(
            src_ref=src, dst_ref=dst, send_sem=send, recv_sem=recv,
            device_id={"cp": device}, device_id_type=pl.DeviceIdType.MESH)

    barrier = pltpu.get_barrier_semaphore()
    for device in [flip(f) for f in (1, 2, 3)] + [group(a) for a in (1, 2, 3)] + [sibling]:
        pl.semaphore_signal(barrier, inc=1, device_id={"cp": device}, device_id_type=pl.DeviceIdType.MESH)
    pl.semaphore_wait(barrier, 7)

    own = [
        pltpu.make_async_copy(k_in.at[batch], kv.at[0, me], loc_sem.at[0]),
        pltpu.make_async_copy(v_in.at[batch], kv.at[1, me], loc_sem.at[1]),
        pltpu.make_async_copy(q_in.at[batch], qs.at[0], loc_sem.at[2]),
        pltpu.make_async_copy(do_in.at[batch], dos.at[0], loc_sem.at[3]),
    ]
    for copy in own:
        copy.start()

    def kv1(f, which):
        src = (k_in, v_in)[which]
        return remote(src.at[flip_batch(f)], kv.at[which, me], kv1_s.at[which, f - 1], kv1_r.at[which, f - 1], flip(f))

    def q_copy(f):
        return remote(q_in.at[flip_batch(f)], qs.at[f], q_sem.at[0, f - 1], q_sem.at[1, f - 1], flip(f))

    def do_copy(f):
        return remote(do_in.at[flip_batch(f)], dos.at[f], do_sem.at[0, f - 1], do_sem.at[1, f - 1], flip(f))

    for f in (1, 2, 3):
        kv1(f, 0).start()
        kv1(f, 1).start()

    def kv2(a, f):
        g = flip(f)
        return remote(kv.at[:, g], kv.at[:, g], kv2_s.at[(a - 1) * 4 + f], kv_r.at[g], group(a))

    def kvf(g, f, a):
        return remote(kv.at[:, g], kv.at[:, g], kvf_s.at[f], kv_r.at[g], group(a))

    def kvd(g):
        return remote(kv.at[:, g], kv.at[:, g], kvd_s.at[g // 2], kv_r.at[g], sibling)

    def member(a, f):
        ax, ay, fx, fy = a % 2, a // 2, f % 2, f // 2
        xa = x + ax * (1 + 4 * qx - 2 * x)
        ya = y + ay * (1 + 4 * qy - 2 * y)
        return ((ya + fy * (3 - 2 * ya)) * side + xa + fx * (3 - 2 * xa)) * 2 + core

    def transpose_rows(src, dst, f):
        for r in range(rows // tile):
            dst[f, :, r * tile:(r + 1) * tile] = src[f, r * tile:(r + 1) * tile, :].T

    def load_chunk(which, j):
        return kv[which, pl.ds(2 * j, 2)].reshape(keys, head_dim)

    def forward(f, j, masked):
        k_blk = load_chunk(0, j)
        vt_blk = load_chunk(1, j).T
        for r in range(rows // tile):
            cols = slice(r * tile, (r + 1) * tile)
            s = dot(k_blk, qt[f, :, cols]) * alpha
            if masked:
                s = s + bias[:, cols]
            m_old = m_s[:, cols]
            m_new = jnp.maximum(m_old, jnp.max(s, axis=0, keepdims=True))
            p = jnp.exp2(s - m_new)
            corr = jnp.exp2(m_old - m_new)
            l_s[:, cols] = l_s[:, cols] * corr + jnp.sum(p.reshape(keys // 8, 8, tile), axis=0)
            m_s[:, cols] = m_new
            ot[:, cols] = ot[:, cols] * corr + dot(vt_blk, p.astype(BF16))

    def scores(f, j, r, k_blk):
        cols = slice(r * tile, (r + 1) * tile)
        s = dot(k_blk, qt[f, :, cols])
        s_s[:, cols] = s
        top_s[:, cols] = jnp.max(s.reshape(keys // 8, 8, tile), axis=0)

    def scores_all(f, j):
        k_blk = load_chunk(0, j)
        for r in range(rows // tile):
            scores(f, j, r, k_blk)

    def weigh(f, j, masked, ahead):
        vt_blk = load_chunk(1, j).T
        k_next = load_chunk(0, j + 1) if ahead else None
        for r in range(rows // tile):
            cols = slice(r * tile, (r + 1) * tile)
            s = s_s[:, cols]
            if masked:
                s = s + bias[:, cols]
                top = jnp.max(s, axis=0, keepdims=True)
            else:
                top = jnp.max(top_s[:, cols], axis=0, keepdims=True)
            m_old = m_s[:, cols]
            m_new = jnp.maximum(m_old, top * alpha)
            p = jnp.exp2(s * alpha - m_new)
            corr = jnp.exp2(m_old - m_new)
            l_s[:, cols] = l_s[:, cols] * corr + jnp.sum(p.reshape(keys // 8, 8, tile), axis=0)
            m_s[:, cols] = m_new
            p_s[:, cols] = p.astype(BF16)
            if ahead:
                scores(f, j + 1, r, k_next)
            ot[:, cols] = ot[:, cols] * corr + dot(vt_blk, p_s[:, cols])

    def o_copy(f):
        return remote(o_st.at[f], out.at[batch], o_sem.at[0, f - 1], o_sem.at[1, f - 1], flip(f))

    def lse_copy(f):
        return remote(lse_st.at[f], lse_out.at[batch], ls_sem.at[0, f - 1], ls_sem.at[1, f - 1], flip(f))

    own_out = [
        pltpu.make_async_copy(o_st.at[0], out.at[batch], loc_sem.at[4]),
        pltpu.make_async_copy(lse_st.at[0], lse_out.at[batch], loc_sem.at[5]),
        pltpu.make_async_copy(dq_st.at[0], dq_out.at[batch], loc_sem.at[6]),
        pltpu.make_async_copy(fin.at[0, 0], dk_out.at[batch], loc_sem.at[7]),
        pltpu.make_async_copy(fin.at[0, 1], dv_out.at[batch], loc_sem.at[8]),
    ]

    def start_slot(f):
        transpose_rows(qs, qt, f)
        m_s[...] = jnp.full(m_s.shape, -jnp.inf, F32)
        l_s[...] = jnp.zeros(l_s.shape, F32)
        ot[...] = jnp.zeros(ot.shape, F32)

    def finish_slot(f):
        total = jnp.sum(l_s[...], axis=0, keepdims=True)
        m_s[...] = m_s[...] + jnp.log2(total)
        l_s[0:1] = 1.0 / total
        lse = m_s[...]
        lse2[f] = lse
        lse_st[f] = lse * LN2
        for r in range(rows // tile):
            cols = slice(r * tile, (r + 1) * tile)
            low = (ot[:, cols] * l_s[0:1, cols]).astype(BF16)
            ot_low[f, :, cols] = low
            o_st[f, cols, :] = low.T

    def transpose_grad(f):
        transpose_rows(dos, dot_t, f)
        dqt[f] = jnp.zeros(dqt.shape[1:], F32)

    def prepare(f):
        transpose_grad(f)
        for r in range(rows // tile):
            cols = slice(r * tile, (r + 1) * tile)
            prod = ot_low[f, :, cols].astype(F32) * dot_t[f, :, cols].astype(F32)
            delta[f, :, cols] = jnp.sum(prod, axis=0, keepdims=True)

    own[2].wait()
    start_slot(0)

    def clear(g, carry):
        dkdv[:, g] = jnp.zeros((2, tokens, head_dim), F32)
        return carry

    lax.fori_loop(0, blocks, clear, 0)

    def bias_rows(i, carry):
        key = lax.broadcasted_iota(jnp.int32, (8, rows), 0) + i * 8 - core * tokens
        token = lax.broadcasted_iota(jnp.int32, (8, rows), 1) // heads
        bias[pl.ds(pl.multiple_of(i * 8, 8), 8)] = jnp.where(key <= token, 0.0, -jnp.inf)
        return carry

    lax.fori_loop(0, keys // 8, bias_rows, 0)
    own[0].wait()
    own[1].wait()

    def spread(f):
        for a in (1, 2):
            kv2(a, f).start()
        kvd(flip(f)).start()

    spread(0)

    def spread_rest(f, carry):
        kv1(f, 0).wait_recv()
        kv1(f, 1).wait_recv()
        spread(f)
        return carry

    lax.fori_loop(1, 4, spread_rest, 0)
    q_copy(1).start()
    q_copy(2).start()

    def wait_block(g):
        remote(kv.at[:, g], kv.at[:, g], kvd_s.at[g // 2], kv_r.at[g], sibling).wait_recv()

    def source(i):
        late = i // 8
        return (1 - late) * (1 + i % 2) + 3 * late, (1 - late) * (i // 2) + late * (i - 8)

    def arrive(i):
        a, f = source(i)
        g = member(a, f)
        wait_block(g)
        kvd(g).start()

        @pl.when(a + (f + f // 2) % 2 == 1)
        def _():
            kvf(g, f, 2).start()

        @pl.when((a - 1) * (2 - (f + f // 2) % 2) == 1)
        def _():
            kvf(g, f, 1).start()

    def use_chunk(g):
        wait_block(g + 1 - 2 * core)
        j = g // 2

        @pl.when(j < me // 2)
        def _():
            forward(0, j, False)

        @pl.when(j == me // 2)
        def _():
            forward(0, j, True)

    def gather_first(i, carry):
        arrive(i)
        use_chunk(flip(i))
        return carry

    def gather_next(i, carry):
        @pl.when(i == 6)
        def _():
            for f in (1, 2):
                q_copy(f).wait_send()
                do_copy(f).start()

        arrive(i)
        use_chunk(member(*source(i - 4)))
        return carry

    def gather_last(i, carry):
        use_chunk(member(*source(i)))
        return carry

    lax.fori_loop(0, 4, gather_first, 0)
    lax.fori_loop(4, 12, gather_next, 0)
    lax.fori_loop(8, 12, gather_last, 0)
    finish_slot(0)
    own_out[0].start()
    own_out[1].start()
    own[3].wait()
    prepare(0)

    def backward(f, j, masked):
        k_blk = load_chunk(0, j)
        v_blk = load_chunk(1, j)
        kt_blk = k_blk.T
        for r in range(rows // tile):
            cols = slice(r * tile, (r + 1) * tile)
            s = dot(k_blk, qt[f, :, cols]) * alpha
            if masked:
                s = s + bias[:, cols]
            p = jnp.exp2(s - lse2[f, :, cols])
            dp = dot(v_blk, dot_t[f, :, cols])
            ds = p * (dp - delta[f, :, cols])
            p_s[:, cols] = p.astype(BF16)
            ds_s[:, cols] = ds.astype(BF16)
        shape = (2, tokens, head_dim)
        dkdv[1, pl.ds(2 * j, 2)] += dot(p_s[...], dos[f]).reshape(shape)
        dkdv[0, pl.ds(2 * j, 2)] += dot(ds_s[...], qs[f]).reshape(shape)
        for r in range(rows // tile):
            cols = slice(r * tile, (r + 1) * tile)
            dqt[f, :, cols] += dot(kt_blk, ds_s[:, cols])

    def dq_copy(f):
        return remote(dq_st.at[f], dq_out.at[batch], dq_sem.at[0, f - 1], dq_sem.at[1, f - 1], flip(f))

    def finish_dq(f):
        for r in range(rows // tile):
            cols = slice(r * tile, (r + 1) * tile)
            dq_st[f, cols, :] = (dqt[f, :, cols] * scale).astype(BF16).T

    def middle_slot(f, carry):
        last = flip(f) // 2

        q_copy(f).wait_recv()

        @pl.when(f == 3)
        def _():
            q_copy(3).wait_send()
            do_copy(3).wait_send()
            pl.semaphore_signal(gate, inc=1, device_id={"cp": sibling}, device_id_type=pl.DeviceIdType.MESH)
            pl.semaphore_wait(gate, 1)
            for other in (1, 2):
                o_copy(other).start()
                lse_copy(other).start()
            for other in (1, 2):
                dq_copy(other).start()

        start_slot(f)

        def forward_body(j, inner):
            weigh(f, j, False, True)
            return inner

        scores_all(f, 0)
        lax.fori_loop(0, last, forward_body, 0)
        weigh(f, last, True, False)
        finish_slot(f)

        do_copy(f).wait_recv()

        @pl.when(f == 1)
        def _():
            do_copy(1).wait_send()
            do_copy(2).wait_send()
            q_copy(3).start()
            do_copy(3).start()

        prepare(f)

        @pl.when(f < 3)
        def _():
            def backward_body(j, inner):
                backward(f, j, False)
                return inner

            lax.fori_loop(0, last, backward_body, 0)
            backward(f, last, True)
            finish_dq(f)

        return carry

    lax.fori_loop(1, 4, middle_slot, 0)
    o_copy(3).start()
    lse_copy(3).start()

    def r1(j):
        return remote(dkdv.at[:, 2 * j + 1 - core], sib.at[:, j], r1_s.at[j], r1_r.at[j], sibling)

    def r2(g, a, f):
        i = (a - 1) * 4 + f
        return remote(dkdv.at[:, g], peer.at[i], r2_s.at[i], r2_r.at[i], group(a))

    def r2_relay(g, a, f):
        return remote(dkdv.at[:, g], relay.at[f], rl_s.at[f], rl_r.at[f], group(a))

    def order(t):
        stage, f = t // 4, t % 4
        first = (f + f // 2) % 2
        half, odd = stage // 2, stage % 2
        a = 3 * (1 - half) * (1 - odd) + (1 + first) * (1 - half) * odd + (2 - first) * half * (1 - odd)
        return member(a, f) // 2, a, f, first

    def reduce_pair(t):
        j, a, f, first = order(t)
        g = 2 * j + core
        r1(j).wait_recv()
        dkdv[:, g] += sib[:, j]

        @pl.when(t // 4 == 0)
        def _():
            r2_relay(g, 1 + first, f).start()

        @pl.when(t // 4 == 1)
        def _():
            r2(g, a, f).start()

    def reduce_group(t, carry):
        j, a, f, first = order(t)
        g = 2 * j + core
        r2_relay(g, a, f).wait_recv()
        dkdv[:, g] += relay[f]
        r2(g, a, f).start()
        return carry

    def final_chunk(t, carry):
        j = order(t)[0]

        def slot(i, inner):
            f = 3 * i
            last = flip(f) // 2

            @pl.when(j < last)
            def _():
                backward(f, j, False)

            @pl.when(j == last)
            def _():
                backward(f, j, True)

            return inner

        lax.fori_loop(0, 2, slot, 0)
        r1(j).start()

        @pl.when(t > 0)
        def _():
            reduce_pair(t - 1)

        return carry

    lax.fori_loop(0, chunks, final_chunk, 0)
    finish_dq(3)
    dq_copy(3).start()
    finish_dq(0)
    own_out[2].start()
    reduce_pair(chunks - 1)
    lax.fori_loop(8, 12, reduce_group, 0)

    def fin_copy(f, which):
        dst = (dk_out, dv_out)[which]
        return remote(fin.at[f, which], dst.at[batch], r3_s.at[which, f - 1], r3_r.at[which, f - 1], flip(f))

    def finish_kv(f):
        g = flip(f)
        for a in (1, 2):
            r2(g, a, f).wait_recv()
        total = dkdv[:, g] + peer[f] + peer[4 + f]
        fin[f, 0] = (total[0] * scale).astype(BF16)
        fin[f, 1] = total[1].astype(BF16)

    for f in (1, 2, 3, 0):
        finish_kv(f)
        if f:
            fin_copy(f, 0).start()
            fin_copy(f, 1).start()
        else:
            own_out[3].start()
            own_out[4].start()

    for f in (1, 2, 3):
        for which in (0, 1):
            kv1(f, which).wait_send()
            fin_copy(f, which).wait()
        o_copy(f).wait()
        lse_copy(f).wait()
        dq_copy(f).wait()
    for copy in own_out:
        copy.wait()

    def drain(i, carry):
        kv2(1 + i // 4, i % 4).wait_send()
        return carry

    lax.fori_loop(0, 8, drain, 0)
    for f in range(4):
        kvf(flip(f), f, 1).wait_send()
        r2(flip(f), 1, f).wait_send()
        r2(flip(f), 2, f).wait_send()
        r2_relay(flip(f), 1, f).wait_send()

    def drain_sibling(j, carry):
        kvd(2 * j + core).wait_send()
        r1(j).wait_send()
        return carry

    lax.fori_loop(0, chunks, drain_sibling, 0)


def output_kernel(out_in, lse_in, dq_in, dk_in, dv_in, out, lse, dq, dk, dv, wide, narrow, sem_in, sem_out):
    batch, rows = lse_in.shape[0], lse_in.shape[2]
    heads, tokens = lse.shape[1], lse.shape[2]
    moves = []
    for i, (src, dst) in enumerate(((out_in, out), (dq_in, dq))):
        for b in range(batch):
            moves.append((src.at[b], wide.at[i, b], dst.at[b]))
    for i, (src, dst) in enumerate(((dk_in, dk), (dv_in, dv))):
        moves.append((src, narrow.at[i], dst))
    steps = [(pltpu.make_async_copy(src, mid, sem_in.at[i]), pltpu.make_async_copy(mid, dst, sem_out.at[i]))
             for i, (src, mid, dst) in enumerate(moves)]
    for load, _ in steps:
        load.start()
    head = lax.broadcasted_iota(jnp.int32, (heads, rows), 0)
    mine = lax.broadcasted_iota(jnp.int32, (heads, rows), 1) % heads == head
    token = lax.broadcasted_iota(jnp.int32, (rows, tokens), 1)
    pick = jnp.where(lax.broadcasted_iota(jnp.int32, (rows, tokens), 0) // heads == token, 1.0, 0.0).astype(BF16)
    for load, store in steps:
        load.wait()
        store.start()
    for b in range(batch):
        rest = jnp.where(mine, lse_in[b], 0.0)
        total = jnp.zeros((heads, tokens), F32)
        for _ in range(3):
            part = rest.astype(BF16)
            total = total + dot(part, pick)
            rest = rest - part.astype(F32)
        lse[b] = total
    for _, store in steps:
        store.wait()


def solution(mesh):
    cp_size = mesh.shape["cp"]

    def attention_shard(queries, keys, values, out_grad):
        batch, tokens, heads, head_dim = queries.shape
        rows = tokens * heads
        q_rows = queries.reshape(batch, rows, head_dim)
        do_rows = out_grad.reshape(batch, rows, head_dim)
        k_rows = keys.reshape(batch, tokens, head_dim)
        v_rows = values.reshape(batch, tokens, head_dim)
        any_spec = pl.BlockSpec(memory_space=pl.ANY)
        dma = pltpu.SemaphoreType.DMA
        block = (tokens, head_dim)
        shapes = [
            jax.ShapeDtypeStruct((batch, rows, head_dim), BF16),
            jax.ShapeDtypeStruct((batch, 1, rows), F32),
            jax.ShapeDtypeStruct((batch, rows, head_dim), BF16),
            jax.ShapeDtypeStruct((batch,) + block, BF16),
            jax.ShapeDtypeStruct((batch,) + block, BF16),
        ]
        scratch = [
            pltpu.VMEM((4, rows, head_dim), BF16),
            pltpu.VMEM((4, rows, head_dim), BF16),
            pltpu.VMEM((4, head_dim, rows), BF16),
            pltpu.VMEM((4, head_dim, rows), BF16),
            pltpu.VMEM((2, cp_size) + block, BF16),
            pltpu.VMEM((head_dim, rows), F32),
            pltpu.VMEM((4, head_dim, rows), BF16),
            pltpu.VMEM((4, rows, head_dim), BF16),
            pltpu.VMEM((1, rows), F32),
            pltpu.VMEM((8, rows), F32),
            pltpu.VMEM((4, 1, rows), F32),
            pltpu.VMEM((4, 1, rows), F32),
            pltpu.VMEM((4, 1, rows), F32),
            pltpu.VMEM((2 * tokens, rows), F32),
            pltpu.VMEM((2 * tokens, rows), F32),
            pltpu.VMEM((8, rows), F32),
            pltpu.VMEM((2 * tokens, rows), BF16),
            pltpu.VMEM((2 * tokens, rows), BF16),
            pltpu.VMEM((4, head_dim, rows), F32),
            pltpu.VMEM((4, rows, head_dim), BF16),
            pltpu.VMEM((2, cp_size) + block, F32),
            pltpu.VMEM((2, cp_size // 2) + block, F32),
            pltpu.VMEM((8, 2) + block, F32),
            pltpu.VMEM((4, 2) + block, F32),
            pltpu.VMEM((4, 2) + block, BF16),
            dma((9,)), dma((2, 3)), dma((2, 3)), dma((8,)), dma((4,)), dma((cp_size // 2,)), dma((cp_size,)),
            dma((2, 3)), dma((2, 3)), dma((2, 3)), dma((2, 3)), dma((2, 3)),
            dma((cp_size // 2,)), dma((cp_size // 2,)), dma((8,)), dma((8,)), dma((4,)), dma((4,)), dma((2, 3)), dma((2, 3)),
            pltpu.SemaphoreType.REGULAR,
        ]
        out, lse, dq, dk, dv = pl.pallas_call(
            attention_kernel,
            out_shape=shapes,
            in_specs=[any_spec] * 4,
            out_specs=[any_spec] * 5,
            scratch_shapes=scratch,
            name="attention",
            compiler_params=pltpu.CompilerParams(
                collective_id=0, has_side_effects=True, vmem_limit_bytes=60 * 1024 * 1024),
        )(q_rows, do_rows, k_rows, v_rows)
        vmem_spec = pl.BlockSpec(memory_space=pltpu.VMEM)
        out, row_lse, dq, dk, dv = pl.pallas_call(
            output_kernel,
            out_shape=[shapes[0], jax.ShapeDtypeStruct((batch, heads, tokens), F32)] + shapes[2:],
            in_specs=[any_spec, vmem_spec, any_spec, any_spec, any_spec],
            out_specs=[any_spec, vmem_spec, any_spec, any_spec, any_spec],
            scratch_shapes=[
                pltpu.VMEM((2, batch, rows, head_dim), BF16), pltpu.VMEM((2, batch) + block, BF16),
                dma((2 * batch + 2,)), dma((2 * batch + 2,))],
            name="outputs",
            compiler_params=pltpu.CompilerParams(vmem_limit_bytes=60 * 1024 * 1024),
        )(out, lse, dq, dk, dv)
        return out.reshape(queries.shape), row_lse, dq.reshape(queries.shape), dk.reshape(keys.shape), dv.reshape(values.shape)

    seq_spec = P("dp", "cp")
    return jax.shard_map(attention_shard, mesh=mesh, in_specs=(seq_spec, seq_spec, seq_spec, seq_spec), out_specs=(seq_spec, P("dp", None, "cp"), seq_spec, seq_spec, seq_spec), check_vma=False)
```

```python
import functools
import math

import jax
import jax.numpy as jnp
from jax import lax
from jax.experimental import pallas as pl
from jax.experimental.pallas import tpu as pltpu
from jax.sharding import PartitionSpec as P

F32 = jnp.float32
BF16 = jnp.bfloat16
LN2 = math.log(2.0)


def dot(lhs, rhs):
    return jnp.dot(lhs, rhs, preferred_element_type=F32)


def attention_kernel(q_in, do_in, k_in, v_in, out, lse_out, dq_out, dk_out, dv_out,
                     qs, dos, qt, dot_t, kv, ot, ot_low, o_st, m_s, l_s, lse2, delta, lse_st, bias, s_s, top_s, p_s, ds_s,
                     dqt, dq_st, dkdv, sib, peer, relay, fin,
                     loc_sem, kv1_s, kv1_r, kv2_s, kvf_s, kvd_s, kv_r, q_sem, do_sem, o_sem, ls_sem, dq_sem,
                     r1_s, r1_r, r2_s, r2_r, rl_s, rl_r, r3_s, r3_r, gate):
    tokens, head_dim = k_in.shape[1], k_in.shape[2]
    rows = q_in.shape[1]
    heads = rows // tokens
    blocks = kv.shape[1]
    chunks = blocks // 2
    keys = 2 * tokens
    side = 4
    scale = head_dim ** -0.5
    alpha = scale / LN2
    tile = min(256, rows)

    me = lax.axis_index("cp")
    core = me % 2
    chip = me // 2
    x, y = chip % side, chip // side
    qx, qy = x // 2, y // 2
    ux, uy = x + qx * (3 - 2 * x), y + qy * (3 - 2 * y)
    batch = 2 * qy + qx
    sibling = me + 1 - 2 * core

    def flip(f):
        fx, fy = f % 2, f // 2
        return ((y + fy * (3 - 2 * y)) * side + x + fx * (3 - 2 * x)) * 2 + core

    def flip_batch(f):
        fx, fy = f % 2, f // 2
        return 2 * (qy + fy * (1 - 2 * qy)) + qx + fx * (1 - 2 * qx)

    def group(a):
        ax, ay = a % 2, a // 2
        return ((y + ay * (1 + 4 * qy - 2 * y)) * side + x + ax * (1 + 4 * qx - 2 * x)) * 2 + core

    def remote(src, dst, send, recv, device):
        return pltpu.make_async_remote_copy(
            src_ref=src, dst_ref=dst, send_sem=send, recv_sem=recv,
            device_id={"cp": device}, device_id_type=pl.DeviceIdType.MESH)

    barrier = pltpu.get_barrier_semaphore()
    for device in [flip(f) for f in (1, 2, 3)] + [group(a) for a in (1, 2, 3)] + [sibling]:
        pl.semaphore_signal(barrier, inc=1, device_id={"cp": device}, device_id_type=pl.DeviceIdType.MESH)
    pl.semaphore_wait(barrier, 7)

    own = [
        pltpu.make_async_copy(k_in.at[batch], kv.at[0, me], loc_sem.at[0]),
        pltpu.make_async_copy(v_in.at[batch], kv.at[1, me], loc_sem.at[1]),
        pltpu.make_async_copy(q_in.at[batch], qs.at[0], loc_sem.at[2]),
        pltpu.make_async_copy(do_in.at[batch], dos.at[0], loc_sem.at[3]),
    ]
    for copy in own:
        copy.start()

    def kv1(f, which):
        src = (k_in, v_in)[which]
        return remote(src.at[flip_batch(f)], kv.at[which, me], kv1_s.at[which, f - 1], kv1_r.at[which, f - 1], flip(f))

    def q_copy(f):
        return remote(q_in.at[flip_batch(f)], qs.at[f], q_sem.at[0, f - 1], q_sem.at[1, f - 1], flip(f))

    def do_copy(f):
        return remote(do_in.at[flip_batch(f)], dos.at[f], do_sem.at[0, f - 1], do_sem.at[1, f - 1], flip(f))

    for f in (1, 2, 3):
        kv1(f, 0).start()
        kv1(f, 1).start()
    q_copy(1).start()
    q_copy(2).start()

    def kv2(a, f):
        g = flip(f)
        return remote(kv.at[:, g], kv.at[:, g], kv2_s.at[(a - 1) * 4 + f], kv_r.at[g], group(a))

    def kvf(g, f, a):
        return remote(kv.at[:, g], kv.at[:, g], kvf_s.at[f], kv_r.at[g], group(a))

    def kvd(g):
        return remote(kv.at[:, g], kv.at[:, g], kvd_s.at[g // 2], kv_r.at[g], sibling)

    def member(a, f):
        ax, ay, fx, fy = a % 2, a // 2, f % 2, f // 2
        xa = x + ax * (1 + 4 * qx - 2 * x)
        ya = y + ay * (1 + 4 * qy - 2 * y)
        return ((ya + fy * (3 - 2 * ya)) * side + xa + fx * (3 - 2 * xa)) * 2 + core

    def transpose_rows(src, dst, f):
        for r in range(rows // tile):
            dst[f, :, r * tile:(r + 1) * tile] = src[f, r * tile:(r + 1) * tile, :].T

    def load_chunk(which, j):
        return kv[which, pl.ds(2 * j, 2)].reshape(keys, head_dim)

    def forward(f, j, masked):
        k_blk = load_chunk(0, j)
        vt_blk = load_chunk(1, j).T
        for r in range(rows // tile):
            cols = slice(r * tile, (r + 1) * tile)
            s = dot(k_blk, qt[f, :, cols]) * alpha
            if masked:
                s = s + bias[:, cols]
            m_old = m_s[:, cols]
            m_new = jnp.maximum(m_old, jnp.max(s, axis=0, keepdims=True))
            p = jnp.exp2(s - m_new)
            corr = jnp.exp2(m_old - m_new)
            l_s[:, cols] = l_s[:, cols] * corr + jnp.sum(p.reshape(keys // 8, 8, tile), axis=0)
            m_s[:, cols] = m_new
            ot[:, cols] = ot[:, cols] * corr + dot(vt_blk, p.astype(BF16))

    def scores(f, j, r, k_blk):
        cols = slice(r * tile, (r + 1) * tile)
        s = dot(k_blk, qt[f, :, cols])
        s_s[:, cols] = s
        top_s[:, cols] = jnp.max(s.reshape(keys // 8, 8, tile), axis=0)

    def scores_all(f, j):
        k_blk = load_chunk(0, j)
        for r in range(rows // tile):
            scores(f, j, r, k_blk)

    def weigh(f, j, masked, ahead):
        vt_blk = load_chunk(1, j).T
        k_next = load_chunk(0, j + 1) if ahead else None
        for r in range(rows // tile):
            cols = slice(r * tile, (r + 1) * tile)
            s = s_s[:, cols]
            if masked:
                s = s + bias[:, cols]
                top = jnp.max(s, axis=0, keepdims=True)
            else:
                top = jnp.max(top_s[:, cols], axis=0, keepdims=True)
            m_old = m_s[:, cols]
            m_new = jnp.maximum(m_old, top * alpha)
            p = jnp.exp2(s * alpha - m_new)
            corr = jnp.exp2(m_old - m_new)
            l_s[:, cols] = l_s[:, cols] * corr + jnp.sum(p.reshape(keys // 8, 8, tile), axis=0)
            m_s[:, cols] = m_new
            p_s[:, cols] = p.astype(BF16)
            if ahead:
                scores(f, j + 1, r, k_next)
            ot[:, cols] = ot[:, cols] * corr + dot(vt_blk, p_s[:, cols])

    def o_copy(f):
        return remote(o_st.at[f], out.at[batch], o_sem.at[0, f - 1], o_sem.at[1, f - 1], flip(f))

    def lse_copy(f):
        return remote(lse_st.at[f], lse_out.at[batch], ls_sem.at[0, f - 1], ls_sem.at[1, f - 1], flip(f))

    own_out = [
        pltpu.make_async_copy(o_st.at[0], out.at[batch], loc_sem.at[4]),
        pltpu.make_async_copy(lse_st.at[0], lse_out.at[batch], loc_sem.at[5]),
        pltpu.make_async_copy(dq_st.at[0], dq_out.at[batch], loc_sem.at[6]),
        pltpu.make_async_copy(fin.at[0, 0], dk_out.at[batch], loc_sem.at[7]),
        pltpu.make_async_copy(fin.at[0, 1], dv_out.at[batch], loc_sem.at[8]),
    ]

    def start_slot(f):
        transpose_rows(qs, qt, f)
        m_s[...] = jnp.full(m_s.shape, -jnp.inf, F32)
        l_s[...] = jnp.zeros(l_s.shape, F32)
        ot[...] = jnp.zeros(ot.shape, F32)

    def finish_slot(f):
        total = jnp.sum(l_s[...], axis=0, keepdims=True)
        m_s[...] = m_s[...] + jnp.log2(total)
        l_s[0:1] = 1.0 / total
        lse = m_s[...]
        lse2[f] = lse
        lse_st[f] = lse * LN2
        for r in range(rows // tile):
            cols = slice(r * tile, (r + 1) * tile)
            low = (ot[:, cols] * l_s[0:1, cols]).astype(BF16)
            ot_low[f, :, cols] = low
            o_st[f, cols, :] = low.T

    def transpose_grad(f):
        transpose_rows(dos, dot_t, f)
        dqt[f] = jnp.zeros(dqt.shape[1:], F32)

    def prepare(f):
        transpose_grad(f)
        for r in range(rows // tile):
            cols = slice(r * tile, (r + 1) * tile)
            prod = ot_low[f, :, cols].astype(F32) * dot_t[f, :, cols].astype(F32)
            delta[f, :, cols] = jnp.sum(prod, axis=0, keepdims=True)

    own[2].wait()
    start_slot(0)

    def clear(g, carry):
        dkdv[:, g] = jnp.zeros((2, tokens, head_dim), F32)
        return carry

    lax.fori_loop(0, blocks, clear, 0)

    def bias_rows(i, carry):
        key = lax.broadcasted_iota(jnp.int32, (8, rows), 0) + i * 8 - core * tokens
        token = lax.broadcasted_iota(jnp.int32, (8, rows), 1) // heads
        bias[pl.ds(pl.multiple_of(i * 8, 8), 8)] = jnp.where(key <= token, 0.0, -jnp.inf)
        return carry

    lax.fori_loop(0, keys // 8, bias_rows, 0)
    own[0].wait()
    own[1].wait()

    def spread(f):
        for a in (1, 2):
            kv2(a, f).start()
        kvd(flip(f)).start()

    spread(0)

    def spread_rest(f, carry):
        kv1(f, 0).wait_recv()
        kv1(f, 1).wait_recv()
        spread(f)
        return carry

    lax.fori_loop(1, 4, spread_rest, 0)
    do_copy(1).start()
    do_copy(2).start()

    def wait_block(g):
        remote(kv.at[:, g], kv.at[:, g], kvd_s.at[g // 2], kv_r.at[g], sibling).wait_recv()

    def source(i):
        late = i // 8
        return (1 - late) * (1 + i % 2) + 3 * late, (1 - late) * (i // 2) + late * (i - 8)

    def arrive(i):
        a, f = source(i)
        g = member(a, f)
        wait_block(g)
        kvd(g).start()

        @pl.when(a + (f + f // 2) % 2 == 1)
        def _():
            kvf(g, f, 2).start()

        @pl.when((a - 1) * (2 - (f + f // 2) % 2) == 1)
        def _():
            kvf(g, f, 1).start()

    def use_chunk(g):
        wait_block(g + 1 - 2 * core)
        j = g // 2

        @pl.when(j < me // 2)
        def _():
            forward(0, j, False)

        @pl.when(j == me // 2)
        def _():
            forward(0, j, True)

    def gather_first(i, carry):
        arrive(i)
        use_chunk(flip(i))
        return carry

    def gather_next(i, carry):
        arrive(i)
        use_chunk(member(*source(i - 4)))
        return carry

    def gather_last(i, carry):
        use_chunk(member(*source(i)))
        return carry

    lax.fori_loop(0, 4, gather_first, 0)
    lax.fori_loop(4, 12, gather_next, 0)
    lax.fori_loop(8, 12, gather_last, 0)
    finish_slot(0)
    own_out[0].start()
    own_out[1].start()
    own[3].wait()
    prepare(0)

    def backward(f, j, masked):
        k_blk = load_chunk(0, j)
        v_blk = load_chunk(1, j)
        kt_blk = k_blk.T
        for r in range(rows // tile):
            cols = slice(r * tile, (r + 1) * tile)
            s = dot(k_blk, qt[f, :, cols]) * alpha
            if masked:
                s = s + bias[:, cols]
            p = jnp.exp2(s - lse2[f, :, cols])
            dp = dot(v_blk, dot_t[f, :, cols])
            ds = p * (dp - delta[f, :, cols])
            p_s[:, cols] = p.astype(BF16)
            ds_s[:, cols] = ds.astype(BF16)
        shape = (2, tokens, head_dim)
        dkdv[1, pl.ds(2 * j, 2)] += dot(p_s[...], dos[f]).reshape(shape)
        dkdv[0, pl.ds(2 * j, 2)] += dot(ds_s[...], qs[f]).reshape(shape)
        for r in range(rows // tile):
            cols = slice(r * tile, (r + 1) * tile)
            dqt[f, :, cols] += dot(kt_blk, ds_s[:, cols])

    def dq_copy(f):
        return remote(dq_st.at[f], dq_out.at[batch], dq_sem.at[0, f - 1], dq_sem.at[1, f - 1], flip(f))

    def finish_dq(f):
        for r in range(rows // tile):
            cols = slice(r * tile, (r + 1) * tile)
            dq_st[f, cols, :] = (dqt[f, :, cols] * scale).astype(BF16).T

    def middle_slot(f, carry):
        last = flip(f) // 2

        q_copy(f).wait_recv()

        @pl.when(f == 3)
        def _():
            q_copy(3).wait_send()
            do_copy(3).wait_send()
            pl.semaphore_signal(gate, inc=1, device_id={"cp": sibling}, device_id_type=pl.DeviceIdType.MESH)
            pl.semaphore_wait(gate, 1)
            for other in (1, 2):
                o_copy(other).start()
                lse_copy(other).start()
            for other in (1, 2):
                dq_copy(other).start()

        start_slot(f)

        def forward_body(j, inner):
            weigh(f, j, False, True)
            return inner

        scores_all(f, 0)
        lax.fori_loop(0, last, forward_body, 0)
        weigh(f, last, True, False)
        finish_slot(f)

        do_copy(f).wait_recv()

        @pl.when(f == 1)
        def _():
            do_copy(1).wait_send()
            do_copy(2).wait_send()
            q_copy(3).start()
            do_copy(3).start()

        prepare(f)

        @pl.when(f < 3)
        def _():
            def backward_body(j, inner):
                backward(f, j, False)
                return inner

            lax.fori_loop(0, last, backward_body, 0)
            backward(f, last, True)
            finish_dq(f)

        return carry

    lax.fori_loop(1, 4, middle_slot, 0)
    o_copy(3).start()
    lse_copy(3).start()

    def r1(j):
        return remote(dkdv.at[:, 2 * j + 1 - core], sib.at[:, j], r1_s.at[j], r1_r.at[j], sibling)

    def r2(g, a, f):
        i = (a - 1) * 4 + f
        return remote(dkdv.at[:, g], peer.at[i], r2_s.at[i], r2_r.at[i], group(a))

    def r2_relay(g, a, f):
        return remote(dkdv.at[:, g], relay.at[f], rl_s.at[f], rl_r.at[f], group(a))

    def order(t):
        stage, f = t // 4, t % 4
        first = (f + f // 2) % 2
        half, odd = stage // 2, stage % 2
        a = 3 * (1 - half) * (1 - odd) + (1 + first) * (1 - half) * odd + (2 - first) * half * (1 - odd)
        return member(a, f) // 2, a, f, first

    def reduce_pair(t):
        j, a, f, first = order(t)
        g = 2 * j + core
        r1(j).wait_recv()
        dkdv[:, g] += sib[:, j]

        @pl.when(t // 4 == 0)
        def _():
            r2_relay(g, 1 + first, f).start()

        @pl.when(t // 4 == 1)
        def _():
            r2(g, a, f).start()

    def reduce_group(t, carry):
        j, a, f, first = order(t)
        g = 2 * j + core
        r2_relay(g, a, f).wait_recv()
        dkdv[:, g] += relay[f]
        r2(g, a, f).start()
        return carry

    def final_chunk(t, carry):
        j = order(t)[0]

        def slot(i, inner):
            f = 3 * i
            last = flip(f) // 2

            @pl.when(j < last)
            def _():
                backward(f, j, False)

            @pl.when(j == last)
            def _():
                backward(f, j, True)

            return inner

        lax.fori_loop(0, 2, slot, 0)
        r1(j).start()

        @pl.when(t > 0)
        def _():
            reduce_pair(t - 1)

        return carry

    lax.fori_loop(0, chunks, final_chunk, 0)
    finish_dq(3)
    dq_copy(3).start()
    finish_dq(0)
    own_out[2].start()
    reduce_pair(chunks - 1)
    lax.fori_loop(8, 12, reduce_group, 0)

    def fin_copy(f, which):
        dst = (dk_out, dv_out)[which]
        return remote(fin.at[f, which], dst.at[batch], r3_s.at[which, f - 1], r3_r.at[which, f - 1], flip(f))

    def finish_kv(f):
        g = flip(f)
        for a in (1, 2):
            r2(g, a, f).wait_recv()
        total = dkdv[:, g] + peer[f] + peer[4 + f]
        fin[f, 0] = (total[0] * scale).astype(BF16)
        fin[f, 1] = total[1].astype(BF16)

    for f in (1, 2, 3, 0):
        finish_kv(f)
        if f:
            fin_copy(f, 0).start()
            fin_copy(f, 1).start()
        else:
            own_out[3].start()
            own_out[4].start()

    for f in (1, 2, 3):
        for which in (0, 1):
            kv1(f, which).wait_send()
            fin_copy(f, which).wait()
        if f < 3:
            q_copy(f).wait_send()
        o_copy(f).wait()
        lse_copy(f).wait()
        dq_copy(f).wait()
    for copy in own_out:
        copy.wait()

    def drain(i, carry):
        kv2(1 + i // 4, i % 4).wait_send()
        return carry

    lax.fori_loop(0, 8, drain, 0)
    for f in range(4):
        kvf(flip(f), f, 1).wait_send()
        r2(flip(f), 1, f).wait_send()
        r2(flip(f), 2, f).wait_send()
        r2_relay(flip(f), 1, f).wait_send()

    def drain_sibling(j, carry):
        kvd(2 * j + core).wait_send()
        r1(j).wait_send()
        return carry

    lax.fori_loop(0, chunks, drain_sibling, 0)


def output_kernel(out_in, lse_in, dq_in, dk_in, dv_in, out, lse, dq, dk, dv, wide, narrow, rows_s, lse_s, sem_in, sem_out):
    batch, rows = lse_in.shape[0], lse_in.shape[2]
    heads, tokens = lse.shape[1], lse.shape[2]
    moves = []
    for i, (src, dst) in enumerate(((out_in, out), (dq_in, dq))):
        for b in range(batch):
            moves.append((src.at[b], wide.at[i, b], dst.at[b]))
    for i, (src, dst) in enumerate(((dk_in, dk), (dv_in, dv))):
        moves.append((src, narrow.at[i], dst))
    steps = [(pltpu.make_async_copy(src, mid, sem_in.at[i]), pltpu.make_async_copy(mid, dst, sem_out.at[i]))
             for i, (src, mid, dst) in enumerate(moves)]
    last = len(steps)
    lse_load = pltpu.make_async_copy(lse_in, rows_s, sem_in.at[last])
    lse_store = pltpu.make_async_copy(lse_s, lse, sem_out.at[last])
    lse_load.start()
    for load, _ in steps:
        load.start()
    lse_load.wait()
    head = lax.broadcasted_iota(jnp.int32, (heads, rows), 0)
    mine = lax.broadcasted_iota(jnp.int32, (heads, rows), 1) % heads == head
    token = lax.broadcasted_iota(jnp.int32, (rows, tokens), 1)
    pick = jnp.where(lax.broadcasted_iota(jnp.int32, (rows, tokens), 0) // heads == token, 1.0, 0.0).astype(BF16)
    rest = jnp.concatenate([jnp.where(mine, rows_s[b], 0.0) for b in range(batch)], axis=0)
    total = jnp.zeros((batch * heads, tokens), F32)
    for _ in range(3):
        part = rest.astype(BF16)
        total = total + dot(part, pick)
        rest = rest - part.astype(F32)
    lse_s[...] = total.reshape(batch, heads, tokens)
    for i, (load, store) in enumerate(steps):
        load.wait()
        store.start()
        if i == 3:
            lse_store.start()
    lse_store.wait()
    for _, store in steps:
        store.wait()


def solution(mesh):
    cp_size = mesh.shape["cp"]

    def attention_shard(queries, keys, values, out_grad):
        batch, tokens, heads, head_dim = queries.shape
        rows = tokens * heads
        q_rows = queries.reshape(batch, rows, head_dim)
        do_rows = out_grad.reshape(batch, rows, head_dim)
        k_rows = keys.reshape(batch, tokens, head_dim)
        v_rows = values.reshape(batch, tokens, head_dim)
        any_spec = pl.BlockSpec(memory_space=pl.ANY)
        dma = pltpu.SemaphoreType.DMA
        block = (tokens, head_dim)
        shapes = [
            jax.ShapeDtypeStruct((batch, rows, head_dim), BF16),
            jax.ShapeDtypeStruct((batch, 1, rows), F32),
            jax.ShapeDtypeStruct((batch, rows, head_dim), BF16),
            jax.ShapeDtypeStruct((batch,) + block, BF16),
            jax.ShapeDtypeStruct((batch,) + block, BF16),
        ]
        scratch = [
            pltpu.VMEM((4, rows, head_dim), BF16),
            pltpu.VMEM((4, rows, head_dim), BF16),
            pltpu.VMEM((4, head_dim, rows), BF16),
            pltpu.VMEM((4, head_dim, rows), BF16),
            pltpu.VMEM((2, cp_size) + block, BF16),
            pltpu.VMEM((head_dim, rows), F32),
            pltpu.VMEM((4, head_dim, rows), BF16),
            pltpu.VMEM((4, rows, head_dim), BF16),
            pltpu.VMEM((1, rows), F32),
            pltpu.VMEM((8, rows), F32),
            pltpu.VMEM((4, 1, rows), F32),
            pltpu.VMEM((4, 1, rows), F32),
            pltpu.VMEM((4, 1, rows), F32),
            pltpu.VMEM((2 * tokens, rows), F32),
            pltpu.VMEM((2 * tokens, rows), F32),
            pltpu.VMEM((8, rows), F32),
            pltpu.VMEM((2 * tokens, rows), BF16),
            pltpu.VMEM((2 * tokens, rows), BF16),
            pltpu.VMEM((4, head_dim, rows), F32),
            pltpu.VMEM((4, rows, head_dim), BF16),
            pltpu.VMEM((2, cp_size) + block, F32),
            pltpu.VMEM((2, cp_size // 2) + block, F32),
            pltpu.VMEM((8, 2) + block, F32),
            pltpu.VMEM((4, 2) + block, F32),
            pltpu.VMEM((4, 2) + block, BF16),
            dma((9,)), dma((2, 3)), dma((2, 3)), dma((8,)), dma((4,)), dma((cp_size // 2,)), dma((cp_size,)),
            dma((2, 3)), dma((2, 3)), dma((2, 3)), dma((2, 3)), dma((2, 3)),
            dma((cp_size // 2,)), dma((cp_size // 2,)), dma((8,)), dma((8,)), dma((4,)), dma((4,)), dma((2, 3)), dma((2, 3)),
            pltpu.SemaphoreType.REGULAR,
        ]
        out, lse, dq, dk, dv = pl.pallas_call(
            attention_kernel,
            out_shape=shapes,
            in_specs=[any_spec] * 4,
            out_specs=[any_spec] * 5,
            scratch_shapes=scratch,
            name="attention",
            compiler_params=pltpu.CompilerParams(
                collective_id=0, has_side_effects=True, vmem_limit_bytes=60 * 1024 * 1024),
        )(q_rows, do_rows, k_rows, v_rows)
        out, row_lse, dq, dk, dv = pl.pallas_call(
            output_kernel,
            out_shape=[shapes[0], jax.ShapeDtypeStruct((batch, heads, tokens), F32)] + shapes[2:],
            in_specs=[any_spec] * 5,
            out_specs=[any_spec] * 5,
            scratch_shapes=[
                pltpu.VMEM((2, batch, rows, head_dim), BF16), pltpu.VMEM((2, batch) + block, BF16),
                pltpu.VMEM((batch, 1, rows), F32), pltpu.VMEM((batch, heads, tokens), F32),
                dma((2 * batch + 3,)), dma((2 * batch + 3,))],
            name="outputs",
            compiler_params=pltpu.CompilerParams(vmem_limit_bytes=60 * 1024 * 1024),
        )(out, lse, dq, dk, dv)
        return out.reshape(queries.shape), row_lse, dq.reshape(queries.shape), dk.reshape(keys.shape), dv.reshape(values.shape)

    seq_spec = P("dp", "cp")
    return jax.shard_map(attention_shard, mesh=mesh, in_specs=(seq_spec, seq_spec, seq_spec, seq_spec), out_specs=(seq_spec, P("dp", None, "cp"), seq_spec, seq_spec, seq_spec), check_vma=False)
```

```python
import math

import jax
import jax.numpy as jnp
from jax import lax
from jax.experimental import pallas as pl
from jax.experimental.pallas import tpu as pltpu
from jax.sharding import PartitionSpec as P

F32 = jnp.float32
BF16 = jnp.bfloat16
LN2 = math.log(2.0)


def dot(lhs, rhs):
    return jnp.dot(lhs, rhs, preferred_element_type=F32)


def attention_kernel(q_in, do_in, k_in, v_in, out, lse_out, dq_out, dk_out, dv_out,
                     qs, dos, qt, dot_t, kv, ot, ot_low, o_st, m_s, l_s, lse2, delta, lse_st, bias, s_s, top_s, p_s, ds_s,
                     dqt, dq_st, dkdv, sib, peer, relay, fin,
                     loc_sem, kv1_s, kv1_r, kv2_s, kvf_s, kvd_s, kv_r, q_sem, do_sem, o_sem, ls_sem, dq_sem,
                     r1_s, r1_r, r2_s, r2_r, rl_s, rl_r, r3_s, r3_r, gate):
    tokens, head_dim = k_in.shape[1], k_in.shape[2]
    rows = q_in.shape[1]
    heads = rows // tokens
    blocks = kv.shape[1]
    chunks = blocks // 2
    keys = 2 * tokens
    side = math.isqrt(chunks)
    scale = head_dim ** -0.5
    alpha = scale / LN2
    tile = min(256, rows)

    me = lax.axis_index("cp")
    core = me % 2
    chip = me // 2
    x, y = chip % side, chip // side
    qx, qy = x // 2, y // 2
    ux, uy = x + qx * (3 - 2 * x), y + qy * (3 - 2 * y)
    batch = 2 * qy + qx
    sibling = me + 1 - 2 * core

    def flip(f):
        fx, fy = f % 2, f // 2
        return ((y + fy * (3 - 2 * y)) * side + x + fx * (3 - 2 * x)) * 2 + core

    def flip_batch(f):
        fx, fy = f % 2, f // 2
        return 2 * (qy + fy * (1 - 2 * qy)) + qx + fx * (1 - 2 * qx)

    def group(a):
        ax, ay = a % 2, a // 2
        return ((y + ay * (1 + 4 * qy - 2 * y)) * side + x + ax * (1 + 4 * qx - 2 * x)) * 2 + core

    def remote(src, dst, send, recv, device):
        return pltpu.make_async_remote_copy(
            src_ref=src, dst_ref=dst, send_sem=send, recv_sem=recv,
            device_id={"cp": device}, device_id_type=pl.DeviceIdType.MESH)

    barrier = pltpu.get_barrier_semaphore()
    for device in [flip(f) for f in (1, 2, 3)] + [group(a) for a in (1, 2, 3)] + [sibling]:
        pl.semaphore_signal(barrier, inc=1, device_id={"cp": device}, device_id_type=pl.DeviceIdType.MESH)
    pl.semaphore_wait(barrier, 7)

    own = [
        pltpu.make_async_copy(k_in.at[batch], kv.at[0, me], loc_sem.at[0]),
        pltpu.make_async_copy(v_in.at[batch], kv.at[1, me], loc_sem.at[1]),
        pltpu.make_async_copy(q_in.at[batch], qs.at[0], loc_sem.at[2]),
        pltpu.make_async_copy(do_in.at[batch], dos.at[0], loc_sem.at[3]),
    ]
    for copy in own:
        copy.start()

    def kv1(f, which):
        src = (k_in, v_in)[which]
        return remote(src.at[flip_batch(f)], kv.at[which, me], kv1_s.at[which, f - 1], kv1_r.at[which, f - 1], flip(f))

    def q_copy(f):
        return remote(q_in.at[flip_batch(f)], qs.at[f], q_sem.at[0, f - 1], q_sem.at[1, f - 1], flip(f))

    def do_copy(f):
        return remote(do_in.at[flip_batch(f)], dos.at[f], do_sem.at[0, f - 1], do_sem.at[1, f - 1], flip(f))

    for f in (1, 2, 3):
        kv1(f, 0).start()
        kv1(f, 1).start()
    q_copy(1).start()
    q_copy(2).start()

    def kv2(a, f):
        g = flip(f)
        return remote(kv.at[:, g], kv.at[:, g], kv2_s.at[(a - 1) * 4 + f], kv_r.at[g], group(a))

    def kvf(g, f, a):
        return remote(kv.at[:, g], kv.at[:, g], kvf_s.at[f], kv_r.at[g], group(a))

    def kvd(g):
        return remote(kv.at[:, g], kv.at[:, g], kvd_s.at[g // 2], kv_r.at[g], sibling)

    def member(a, f):
        ax, ay, fx, fy = a % 2, a // 2, f % 2, f // 2
        xa = x + ax * (1 + 4 * qx - 2 * x)
        ya = y + ay * (1 + 4 * qy - 2 * y)
        return ((ya + fy * (3 - 2 * ya)) * side + xa + fx * (3 - 2 * xa)) * 2 + core

    def transpose_rows(src, dst, f):
        for r in range(rows // tile):
            dst[f, :, r * tile:(r + 1) * tile] = src[f, r * tile:(r + 1) * tile, :].T

    def load_chunk(which, j):
        return kv[which, pl.ds(2 * j, 2)].reshape(keys, head_dim)

    def forward(f, j, masked):
        k_blk = load_chunk(0, j)
        vt_blk = load_chunk(1, j).T
        for r in range(rows // tile):
            cols = slice(r * tile, (r + 1) * tile)
            s = dot(k_blk, qt[f, :, cols]) * alpha
            if masked:
                s = s + bias[:, cols]
            m_old = m_s[:, cols]
            m_new = jnp.maximum(m_old, jnp.max(s, axis=0, keepdims=True))
            p = jnp.exp2(s - m_new)
            corr = jnp.exp2(m_old - m_new)
            l_s[:, cols] = l_s[:, cols] * corr + jnp.sum(p.reshape(keys // 8, 8, tile), axis=0)
            m_s[:, cols] = m_new
            ot[:, cols] = ot[:, cols] * corr + dot(vt_blk, p.astype(BF16))

    def scores(f, j, r, k_blk):
        cols = slice(r * tile, (r + 1) * tile)
        s = dot(k_blk, qt[f, :, cols])
        s_s[:, cols] = s
        top_s[:, cols] = jnp.max(s.reshape(keys // 8, 8, tile), axis=0)

    def scores_all(f, j):
        k_blk = load_chunk(0, j)
        for r in range(rows // tile):
            scores(f, j, r, k_blk)

    def weigh(f, j, masked, ahead):
        vt_blk = load_chunk(1, j).T
        k_next = load_chunk(0, j + 1) if ahead else None
        for r in range(rows // tile):
            cols = slice(r * tile, (r + 1) * tile)
            s = s_s[:, cols]
            if masked:
                s = s + bias[:, cols]
                top = jnp.max(s, axis=0, keepdims=True)
            else:
                top = jnp.max(top_s[:, cols], axis=0, keepdims=True)
            m_old = m_s[:, cols]
            m_new = jnp.maximum(m_old, top * alpha)
            p = jnp.exp2(s * alpha - m_new)
            corr = jnp.exp2(m_old - m_new)
            l_s[:, cols] = l_s[:, cols] * corr + jnp.sum(p.reshape(keys // 8, 8, tile), axis=0)
            m_s[:, cols] = m_new
            p_s[:, cols] = p.astype(BF16)
            if ahead:
                scores(f, j + 1, r, k_next)
            ot[:, cols] = ot[:, cols] * corr + dot(vt_blk, p_s[:, cols])

    def o_copy(f):
        return remote(o_st.at[f], out.at[batch], o_sem.at[0, f - 1], o_sem.at[1, f - 1], flip(f))

    def lse_copy(f):
        return remote(lse_st.at[f], lse_out.at[batch], ls_sem.at[0, f - 1], ls_sem.at[1, f - 1], flip(f))

    own_out = [
        pltpu.make_async_copy(o_st.at[0], out.at[batch], loc_sem.at[4]),
        pltpu.make_async_copy(lse_st.at[0], lse_out.at[batch], loc_sem.at[5]),
        pltpu.make_async_copy(dq_st.at[0], dq_out.at[batch], loc_sem.at[6]),
        pltpu.make_async_copy(fin.at[0, 0], dk_out.at[batch], loc_sem.at[7]),
        pltpu.make_async_copy(fin.at[0, 1], dv_out.at[batch], loc_sem.at[8]),
    ]

    def start_slot(f):
        transpose_rows(qs, qt, f)
        m_s[...] = jnp.full(m_s.shape, -jnp.inf, F32)
        l_s[...] = jnp.zeros(l_s.shape, F32)
        ot[...] = jnp.zeros(ot.shape, F32)

    def finish_slot(f):
        total = jnp.sum(l_s[...], axis=0, keepdims=True)
        m_s[...] = m_s[...] + jnp.log2(total)
        l_s[0:1] = 1.0 / total
        lse = m_s[...]
        lse2[f] = lse
        lse_st[f] = lse * LN2
        for r in range(rows // tile):
            cols = slice(r * tile, (r + 1) * tile)
            low = (ot[:, cols] * l_s[0:1, cols]).astype(BF16)
            ot_low[f, :, cols] = low
            o_st[f, cols, :] = low.T

    def transpose_grad(f):
        transpose_rows(dos, dot_t, f)
        dqt[f] = jnp.zeros(dqt.shape[1:], F32)

    def prepare(f):
        transpose_grad(f)
        for r in range(rows // tile):
            cols = slice(r * tile, (r + 1) * tile)
            prod = ot_low[f, :, cols].astype(F32) * dot_t[f, :, cols].astype(F32)
            delta[f, :, cols] = jnp.sum(prod, axis=0, keepdims=True)

    own[2].wait()
    start_slot(0)

    def clear(g, carry):
        dkdv[:, g] = jnp.zeros((2, tokens, head_dim), F32)
        return carry

    lax.fori_loop(0, blocks, clear, 0)

    def bias_rows(i, carry):
        key = lax.broadcasted_iota(jnp.int32, (8, rows), 0) + i * 8 - core * tokens
        token = lax.broadcasted_iota(jnp.int32, (8, rows), 1) // heads
        bias[pl.ds(pl.multiple_of(i * 8, 8), 8)] = jnp.where(key <= token, 0.0, -jnp.inf)
        return carry

    lax.fori_loop(0, keys // 8, bias_rows, 0)
    own[0].wait()
    own[1].wait()

    def spread(f):
        for a in (1, 2):
            kv2(a, f).start()
        kvd(flip(f)).start()

    spread(0)

    def spread_rest(f, carry):
        kv1(f, 0).wait_recv()
        kv1(f, 1).wait_recv()
        spread(f)
        return carry

    lax.fori_loop(1, 4, spread_rest, 0)
    do_copy(1).start()
    do_copy(2).start()

    def wait_block(g):
        remote(kv.at[:, g], kv.at[:, g], kvd_s.at[g // 2], kv_r.at[g], sibling).wait_recv()

    def source(i):
        late = i // 8
        return (1 - late) * (1 + i % 2) + 3 * late, (1 - late) * (i // 2) + late * (i - 8)

    def arrive(i):
        a, f = source(i)
        g = member(a, f)
        wait_block(g)
        kvd(g).start()

        @pl.when(a + (f + f // 2) % 2 == 1)
        def _():
            kvf(g, f, 2).start()

        @pl.when((a - 1) * (2 - (f + f // 2) % 2) == 1)
        def _():
            kvf(g, f, 1).start()

    def use_chunk(g):
        wait_block(g + 1 - 2 * core)
        j = g // 2

        @pl.when(j < me // 2)
        def _():
            forward(0, j, False)

        @pl.when(j == me // 2)
        def _():
            forward(0, j, True)

    def gather_first(i, carry):
        arrive(i)
        use_chunk(flip(i))
        return carry

    def gather_next(i, carry):
        arrive(i)
        use_chunk(member(*source(i - 4)))
        return carry

    def gather_last(i, carry):
        use_chunk(member(*source(i)))
        return carry

    lax.fori_loop(0, 4, gather_first, 0)
    lax.fori_loop(4, 12, gather_next, 0)
    lax.fori_loop(8, 12, gather_last, 0)
    finish_slot(0)
    own_out[0].start()
    own_out[1].start()
    own[3].wait()
    prepare(0)

    def backward(f, j, masked):
        k_blk = load_chunk(0, j)
        v_blk = load_chunk(1, j)
        kt_blk = k_blk.T
        for r in range(rows // tile):
            cols = slice(r * tile, (r + 1) * tile)
            s = dot(k_blk, qt[f, :, cols]) * alpha
            if masked:
                s = s + bias[:, cols]
            p = jnp.exp2(s - lse2[f, :, cols])
            dp = dot(v_blk, dot_t[f, :, cols])
            ds = p * (dp - delta[f, :, cols])
            p_s[:, cols] = p.astype(BF16)
            ds_s[:, cols] = ds.astype(BF16)
        shape = (2, tokens, head_dim)
        dkdv[1, pl.ds(2 * j, 2)] += dot(p_s[...], dos[f]).reshape(shape)
        dkdv[0, pl.ds(2 * j, 2)] += dot(ds_s[...], qs[f]).reshape(shape)
        for r in range(rows // tile):
            cols = slice(r * tile, (r + 1) * tile)
            dqt[f, :, cols] += dot(kt_blk, ds_s[:, cols])

    def dq_copy(f):
        return remote(dq_st.at[f], dq_out.at[batch], dq_sem.at[0, f - 1], dq_sem.at[1, f - 1], flip(f))

    def finish_dq(f):
        for r in range(rows // tile):
            cols = slice(r * tile, (r + 1) * tile)
            dq_st[f, cols, :] = (dqt[f, :, cols] * scale).astype(BF16).T

    def middle_slot(f, carry):
        last = flip(f) // 2

        q_copy(f).wait_recv()

        @pl.when(f == 3)
        def _():
            q_copy(3).wait_send()
            do_copy(3).wait_send()
            pl.semaphore_signal(gate, inc=1, device_id={"cp": sibling}, device_id_type=pl.DeviceIdType.MESH)
            pl.semaphore_wait(gate, 1)
            for other in (1, 2):
                o_copy(other).start()
                lse_copy(other).start()
            for other in (1, 2):
                dq_copy(other).start()

        start_slot(f)

        def forward_body(j, inner):
            weigh(f, j, False, True)
            return inner

        scores_all(f, 0)
        lax.fori_loop(0, last, forward_body, 0)
        weigh(f, last, True, False)
        finish_slot(f)

        do_copy(f).wait_recv()

        @pl.when(f == 1)
        def _():
            do_copy(1).wait_send()
            do_copy(2).wait_send()
            q_copy(3).start()
            do_copy(3).start()

        prepare(f)

        @pl.when(f < 3)
        def _():
            def backward_body(j, inner):
                backward(f, j, False)
                return inner

            lax.fori_loop(0, last, backward_body, 0)
            backward(f, last, True)
            finish_dq(f)

        return carry

    lax.fori_loop(1, 4, middle_slot, 0)
    o_copy(3).start()
    lse_copy(3).start()

    def r1(j):
        return remote(dkdv.at[:, 2 * j + 1 - core], sib.at[:, j], r1_s.at[j], r1_r.at[j], sibling)

    def r2(g, a, f):
        i = (a - 1) * 4 + f
        return remote(dkdv.at[:, g], peer.at[i], r2_s.at[i], r2_r.at[i], group(a))

    def r2_relay(g, a, f):
        return remote(dkdv.at[:, g], relay.at[f], rl_s.at[f], rl_r.at[f], group(a))

    def order(t):
        stage, f = t // 4, t % 4
        first = (f + f // 2) % 2
        half, odd = stage // 2, stage % 2
        a = 3 * (1 - half) * (1 - odd) + (1 + first) * (1 - half) * odd + (2 - first) * half * (1 - odd)
        return member(a, f) // 2, a, f, first

    def reduce_pair(t):
        j, a, f, first = order(t)
        g = 2 * j + core
        r1(j).wait_recv()
        dkdv[:, g] += sib[:, j]

        @pl.when(t // 4 == 0)
        def _():
            r2_relay(g, 1 + first, f).start()

        @pl.when(t // 4 == 1)
        def _():
            r2(g, a, f).start()

    def second(f):
        a = 2 - (f + f // 2) % 2
        return r2(2 * (member(a, f) // 2) + core, a, f)

    def reduce_group(f):
        a = 2 - (f + f // 2) % 2
        g = 2 * (member(a, f) // 2) + core
        r2_relay(g, a, f).wait_recv()
        dkdv[:, g] += relay[f]
        second(f).start()

    def final_chunk(t, carry):
        j = order(t)[0]

        def slot(i, inner):
            f = 3 * i
            last = flip(f) // 2

            @pl.when(j < last)
            def _():
                backward(f, j, False)

            @pl.when(j == last)
            def _():
                backward(f, j, True)

            return inner

        lax.fori_loop(0, 2, slot, 0)
        r1(j).start()

        @pl.when(t > 0)
        def _():
            reduce_pair(t - 1)

        return carry

    lax.fori_loop(0, chunks, final_chunk, 0)
    finish_dq(3)
    dq_copy(3).start()
    finish_dq(0)
    own_out[2].start()
    reduce_pair(chunks - 1)
    reduce_group(3)
    reduce_group(1)
    second(3).wait_send()
    second(1).wait_send()
    reduce_group(0)
    reduce_group(2)

    def fin_copy(f, which):
        dst = (dk_out, dv_out)[which]
        return remote(fin.at[f, which], dst.at[batch], r3_s.at[which, f - 1], r3_r.at[which, f - 1], flip(f))

    def finish_kv(f):
        g = flip(f)
        for a in (1, 2):
            r2(g, a, f).wait_recv()
        total = dkdv[:, g] + peer[f] + peer[4 + f]
        fin[f, 0] = (total[0] * scale).astype(BF16)
        fin[f, 1] = total[1].astype(BF16)

    for f in (3, 1, 2, 0):
        finish_kv(f)
        if f:
            fin_copy(f, 0).start()
            fin_copy(f, 1).start()
        else:
            own_out[3].start()
            own_out[4].start()

    for f in (1, 2, 3):
        for which in (0, 1):
            kv1(f, which).wait_send()
            fin_copy(f, which).wait()
        if f < 3:
            q_copy(f).wait_send()
        o_copy(f).wait()
        lse_copy(f).wait()
        dq_copy(f).wait()
    for copy in own_out:
        copy.wait()

    def drain(i, carry):
        kv2(1 + i // 4, i % 4).wait_send()
        return carry

    lax.fori_loop(0, 8, drain, 0)
    for f in range(4):
        kvf(flip(f), f, 1).wait_send()
        r2(flip(f), 1 + (f + f // 2) % 2, f).wait_send()
        if f in (0, 2):
            second(f).wait_send()
        r2_relay(flip(f), 1, f).wait_send()

    def drain_sibling(j, carry):
        kvd(2 * j + core).wait_send()
        r1(j).wait_send()
        return carry

    lax.fori_loop(0, chunks, drain_sibling, 0)


def output_kernel(out_in, lse_in, dq_in, dk_in, dv_in, out, lse, dq, dk, dv, wide, narrow, rows_s, lse_s, sem_in, sem_out):
    batch, rows = lse_in.shape[0], lse_in.shape[2]
    heads, tokens = lse.shape[1], lse.shape[2]
    moves = []
    for i, (src, dst) in enumerate(((out_in, out), (dq_in, dq))):
        for b in range(batch):
            moves.append((src.at[b], wide.at[i, b], dst.at[b]))
    for i, (src, dst) in enumerate(((dk_in, dk), (dv_in, dv))):
        moves.append((src, narrow.at[i], dst))
    steps = [(pltpu.make_async_copy(src, mid, sem_in.at[i]), pltpu.make_async_copy(mid, dst, sem_out.at[i]))
             for i, (src, mid, dst) in enumerate(moves)]
    last = len(steps)
    lse_load = pltpu.make_async_copy(lse_in, rows_s, sem_in.at[last])
    lse_store = pltpu.make_async_copy(lse_s, lse, sem_out.at[last])
    lse_load.start()
    for load, _ in steps:
        load.start()
    lse_load.wait()
    head = lax.broadcasted_iota(jnp.int32, (heads, rows), 0)
    mine = lax.broadcasted_iota(jnp.int32, (heads, rows), 1) % heads == head
    token = lax.broadcasted_iota(jnp.int32, (rows, tokens), 1)
    pick = jnp.where(lax.broadcasted_iota(jnp.int32, (rows, tokens), 0) // heads == token, 1.0, 0.0).astype(BF16)
    rest = jnp.concatenate([jnp.where(mine, rows_s[b], 0.0) for b in range(batch)], axis=0)
    total = jnp.zeros((batch * heads, tokens), F32)
    for _ in range(3):
        part = rest.astype(BF16)
        total = total + dot(part, pick)
        rest = rest - part.astype(F32)
    lse_s[...] = total.reshape(batch, heads, tokens)
    for i, (load, store) in enumerate(steps):
        load.wait()
        store.start()
        if i == 3:
            lse_store.start()
    lse_store.wait()
    for _, store in steps:
        store.wait()


def solution(mesh):
    cp_size = mesh.shape["cp"]

    def attention_shard(queries, keys, values, out_grad):
        batch, tokens, heads, head_dim = queries.shape
        rows = tokens * heads
        q_rows = queries.reshape(batch, rows, head_dim)
        do_rows = out_grad.reshape(batch, rows, head_dim)
        k_rows = keys.reshape(batch, tokens, head_dim)
        v_rows = values.reshape(batch, tokens, head_dim)
        any_spec = pl.BlockSpec(memory_space=pl.ANY)
        dma = pltpu.SemaphoreType.DMA
        block = (tokens, head_dim)
        shapes = [
            jax.ShapeDtypeStruct((batch, rows, head_dim), BF16),
            jax.ShapeDtypeStruct((batch, 1, rows), F32),
            jax.ShapeDtypeStruct((batch, rows, head_dim), BF16),
            jax.ShapeDtypeStruct((batch,) + block, BF16),
            jax.ShapeDtypeStruct((batch,) + block, BF16),
        ]
        scratch = [
            pltpu.VMEM((4, rows, head_dim), BF16),
            pltpu.VMEM((4, rows, head_dim), BF16),
            pltpu.VMEM((4, head_dim, rows), BF16),
            pltpu.VMEM((4, head_dim, rows), BF16),
            pltpu.VMEM((2, cp_size) + block, BF16),
            pltpu.VMEM((head_dim, rows), F32),
            pltpu.VMEM((4, head_dim, rows), BF16),
            pltpu.VMEM((4, rows, head_dim), BF16),
            pltpu.VMEM((1, rows), F32),
            pltpu.VMEM((8, rows), F32),
            pltpu.VMEM((4, 1, rows), F32),
            pltpu.VMEM((4, 1, rows), F32),
            pltpu.VMEM((4, 1, rows), F32),
            pltpu.VMEM((2 * tokens, rows), F32),
            pltpu.VMEM((2 * tokens, rows), F32),
            pltpu.VMEM((8, rows), F32),
            pltpu.VMEM((2 * tokens, rows), BF16),
            pltpu.VMEM((2 * tokens, rows), BF16),
            pltpu.VMEM((4, head_dim, rows), F32),
            pltpu.VMEM((4, rows, head_dim), BF16),
            pltpu.VMEM((2, cp_size) + block, F32),
            pltpu.VMEM((2, cp_size // 2) + block, F32),
            pltpu.VMEM((8, 2) + block, F32),
            pltpu.VMEM((4, 2) + block, F32),
            pltpu.VMEM((4, 2) + block, BF16),
            dma((9,)), dma((2, 3)), dma((2, 3)), dma((8,)), dma((4,)), dma((cp_size // 2,)), dma((cp_size,)),
            dma((2, 3)), dma((2, 3)), dma((2, 3)), dma((2, 3)), dma((2, 3)),
            dma((cp_size // 2,)), dma((cp_size // 2,)), dma((8,)), dma((8,)), dma((4,)), dma((4,)), dma((2, 3)), dma((2, 3)),
            pltpu.SemaphoreType.REGULAR,
        ]
        out, lse, dq, dk, dv = pl.pallas_call(
            attention_kernel,
            out_shape=shapes,
            in_specs=[any_spec] * 4,
            out_specs=[any_spec] * 5,
            scratch_shapes=scratch,
            name="attention",
            compiler_params=pltpu.CompilerParams(
                collective_id=0, has_side_effects=True, vmem_limit_bytes=60 * 1024 * 1024),
        )(q_rows, do_rows, k_rows, v_rows)
        out, row_lse, dq, dk, dv = pl.pallas_call(
            output_kernel,
            out_shape=[shapes[0], jax.ShapeDtypeStruct((batch, heads, tokens), F32)] + shapes[2:],
            in_specs=[any_spec] * 5,
            out_specs=[any_spec] * 5,
            scratch_shapes=[
                pltpu.VMEM((2, batch, rows, head_dim), BF16), pltpu.VMEM((2, batch) + block, BF16),
                pltpu.VMEM((batch, 1, rows), F32), pltpu.VMEM((batch, heads, tokens), F32),
                dma((2 * batch + 3,)), dma((2 * batch + 3,))],
            name="outputs",
            compiler_params=pltpu.CompilerParams(vmem_limit_bytes=60 * 1024 * 1024),
        )(out, lse, dq, dk, dv)
        return out.reshape(queries.shape), row_lse, dq.reshape(queries.shape), dk.reshape(keys.shape), dv.reshape(values.shape)

    seq_spec = P("dp", "cp")
    return jax.shard_map(attention_shard, mesh=mesh, in_specs=(seq_spec, seq_spec, seq_spec, seq_spec), out_specs=(seq_spec, P("dp", None, "cp"), seq_spec, seq_spec, seq_spec), check_vma=False)
```

```python
import math

import jax
import jax.numpy as jnp
from jax import lax
from jax.experimental import pallas as pl
from jax.experimental.pallas import tpu as pltpu
from jax.sharding import PartitionSpec as P

F32 = jnp.float32
BF16 = jnp.bfloat16
LN2 = math.log(2.0)


def dot(lhs, rhs):
    return jnp.dot(lhs, rhs, preferred_element_type=F32)


def attention_kernel(q_in, do_in, k_in, v_in, out, lse_out, dq_out, dk_out, dv_out,
                     qs, dos, qt, dot_t, kv, ot, ot_low, o_st, m_s, l_s, lse2, delta, lse_st, bias, s_s, top_s, p_s, ds_s,
                     dqt, dq_st, dkdv, sib, peer, relay, fin,
                     loc_sem, kv1_s, kv1_r, kv2_s, kvf_s, kvd_s, kv_r, q_sem, do_sem, o_sem, ls_sem, dq_sem,
                     r1_s, r1_r, r2_s, r2_r, rl_s, rl_r, r3_s, r3_r, gate):
    tokens, head_dim = k_in.shape[1], k_in.shape[2]
    rows = q_in.shape[1]
    heads = rows // tokens
    blocks = kv.shape[1]
    chunks = blocks // 2
    keys = 2 * tokens
    side = math.isqrt(chunks)
    scale = head_dim ** -0.5
    alpha = scale / LN2
    tile = min(256, rows)

    me = lax.axis_index("cp")
    core = me % 2
    chip = me // 2
    x, y = chip % side, chip // side
    qx, qy = x // 2, y // 2
    ux, uy = x + qx * (3 - 2 * x), y + qy * (3 - 2 * y)
    batch = 2 * qy + qx
    sibling = me + 1 - 2 * core

    def flip(f):
        fx, fy = f % 2, f // 2
        return ((y + fy * (3 - 2 * y)) * side + x + fx * (3 - 2 * x)) * 2 + core

    def flip_batch(f):
        fx, fy = f % 2, f // 2
        return 2 * (qy + fy * (1 - 2 * qy)) + qx + fx * (1 - 2 * qx)

    def group(a):
        ax, ay = a % 2, a // 2
        return ((y + ay * (1 + 4 * qy - 2 * y)) * side + x + ax * (1 + 4 * qx - 2 * x)) * 2 + core

    def remote(src, dst, send, recv, device):
        return pltpu.make_async_remote_copy(
            src_ref=src, dst_ref=dst, send_sem=send, recv_sem=recv,
            device_id={"cp": device}, device_id_type=pl.DeviceIdType.MESH)

    barrier = pltpu.get_barrier_semaphore()
    for device in [flip(f) for f in (1, 2, 3)] + [group(a) for a in (1, 2, 3)] + [sibling]:
        pl.semaphore_signal(barrier, inc=1, device_id={"cp": device}, device_id_type=pl.DeviceIdType.MESH)
    pl.semaphore_wait(barrier, 7)

    own = [
        pltpu.make_async_copy(k_in.at[batch], kv.at[0, me], loc_sem.at[0]),
        pltpu.make_async_copy(v_in.at[batch], kv.at[1, me], loc_sem.at[1]),
        pltpu.make_async_copy(q_in.at[batch], qs.at[0], loc_sem.at[2]),
        pltpu.make_async_copy(do_in.at[batch], dos.at[0], loc_sem.at[3]),
    ]
    for copy in own:
        copy.start()

    def kv1(f, which):
        src = (k_in, v_in)[which]
        return remote(src.at[flip_batch(f)], kv.at[which, me], kv1_s.at[which, f - 1], kv1_r.at[which, f - 1], flip(f))

    def q_copy(f):
        return remote(q_in.at[flip_batch(f)], qs.at[f], q_sem.at[0, f - 1], q_sem.at[1, f - 1], flip(f))

    def do_copy(f):
        return remote(do_in.at[flip_batch(f)], dos.at[f], do_sem.at[0, f - 1], do_sem.at[1, f - 1], flip(f))

    for f in (1, 2, 3):
        kv1(f, 0).start()
        kv1(f, 1).start()
    q_copy(1).start()
    q_copy(2).start()

    def kv2(a, f):
        g = flip(f)
        return remote(kv.at[:, g], kv.at[:, g], kv2_s.at[(a - 1) * 4 + f], kv_r.at[g], group(a))

    def kvf(g, f, a):
        return remote(kv.at[:, g], kv.at[:, g], kvf_s.at[f], kv_r.at[g], group(a))

    def kvd(g):
        return remote(kv.at[:, g], kv.at[:, g], kvd_s.at[g // 2], kv_r.at[g], sibling)

    def member(a, f):
        ax, ay, fx, fy = a % 2, a // 2, f % 2, f // 2
        xa = x + ax * (1 + 4 * qx - 2 * x)
        ya = y + ay * (1 + 4 * qy - 2 * y)
        return ((ya + fy * (3 - 2 * ya)) * side + xa + fx * (3 - 2 * xa)) * 2 + core

    def transpose_rows(src, dst, f):
        for r in range(rows // tile):
            dst[f, :, r * tile:(r + 1) * tile] = src[f, r * tile:(r + 1) * tile, :].T

    def load_chunk(which, j):
        return kv[which, pl.ds(2 * j, 2)].reshape(keys, head_dim)

    def forward(f, j, masked):
        k_blk = load_chunk(0, j)
        vt_blk = load_chunk(1, j).T
        for r in range(rows // tile):
            cols = slice(r * tile, (r + 1) * tile)
            s = dot(k_blk, qt[f, :, cols]) * alpha
            if masked:
                s = s + bias[:, cols]
            m_old = m_s[:, cols]
            m_new = jnp.maximum(m_old, jnp.max(s, axis=0, keepdims=True))
            p = jnp.exp2(s - m_new)
            corr = jnp.exp2(m_old - m_new)
            l_s[:, cols] = l_s[:, cols] * corr + jnp.sum(p.reshape(keys // 8, 8, tile), axis=0)
            m_s[:, cols] = m_new
            ot[:, cols] = ot[:, cols] * corr + dot(vt_blk, p.astype(BF16))

    def scores(f, j, r, k_blk):
        cols = slice(r * tile, (r + 1) * tile)
        s = dot(k_blk, qt[f, :, cols])
        s_s[:, cols] = s
        top_s[:, cols] = jnp.max(s.reshape(keys // 8, 8, tile), axis=0)

    def scores_all(f, j):
        k_blk = load_chunk(0, j)
        for r in range(rows // tile):
            scores(f, j, r, k_blk)

    def weigh(f, j, masked, ahead):
        vt_blk = load_chunk(1, j).T
        k_next = load_chunk(0, j + 1) if ahead else None
        for r in range(rows // tile):
            cols = slice(r * tile, (r + 1) * tile)
            s = s_s[:, cols]
            if masked:
                s = s + bias[:, cols]
                top = jnp.max(s, axis=0, keepdims=True)
            else:
                top = jnp.max(top_s[:, cols], axis=0, keepdims=True)
            m_old = m_s[:, cols]
            m_new = jnp.maximum(m_old, top * alpha)
            p = jnp.exp2(s * alpha - m_new)
            corr = jnp.exp2(m_old - m_new)
            l_s[:, cols] = l_s[:, cols] * corr + jnp.sum(p.reshape(keys // 8, 8, tile), axis=0)
            m_s[:, cols] = m_new
            p_s[:, cols] = p.astype(BF16)
            if ahead:
                scores(f, j + 1, r, k_next)
            ot[:, cols] = ot[:, cols] * corr + dot(vt_blk, p_s[:, cols])

    def o_copy(f):
        return remote(o_st.at[f], out.at[batch], o_sem.at[0, f - 1], o_sem.at[1, f - 1], flip(f))

    def lse_copy(f):
        return remote(lse_st.at[f], lse_out.at[batch], ls_sem.at[0, f - 1], ls_sem.at[1, f - 1], flip(f))

    own_out = [
        pltpu.make_async_copy(o_st.at[0], out.at[batch], loc_sem.at[4]),
        pltpu.make_async_copy(lse_st.at[0], lse_out.at[batch], loc_sem.at[5]),
        pltpu.make_async_copy(dq_st.at[0], dq_out.at[batch], loc_sem.at[6]),
        pltpu.make_async_copy(fin.at[0, 0], dk_out.at[batch], loc_sem.at[7]),
        pltpu.make_async_copy(fin.at[0, 1], dv_out.at[batch], loc_sem.at[8]),
    ]

    def start_slot(f):
        transpose_rows(qs, qt, f)
        m_s[...] = jnp.full(m_s.shape, -jnp.inf, F32)
        l_s[...] = jnp.zeros(l_s.shape, F32)
        ot[...] = jnp.zeros(ot.shape, F32)

    def finish_slot(f):
        total = jnp.sum(l_s[...], axis=0, keepdims=True)
        m_s[...] = m_s[...] + jnp.log2(total)
        l_s[0:1] = 1.0 / total
        lse = m_s[...]
        lse2[f] = lse
        lse_st[f] = lse * LN2
        for r in range(rows // tile):
            cols = slice(r * tile, (r + 1) * tile)
            low = (ot[:, cols] * l_s[0:1, cols]).astype(BF16)
            ot_low[f, :, cols] = low
            o_st[f, cols, :] = low.T

    def transpose_grad(f):
        transpose_rows(dos, dot_t, f)
        dqt[f] = jnp.zeros(dqt.shape[1:], F32)

    def prepare(f):
        transpose_grad(f)
        for r in range(rows // tile):
            cols = slice(r * tile, (r + 1) * tile)
            prod = ot_low[f, :, cols].astype(F32) * dot_t[f, :, cols].astype(F32)
            delta[f, :, cols] = jnp.sum(prod, axis=0, keepdims=True)

    own[2].wait()
    start_slot(0)

    def clear(g, carry):
        dkdv[:, g] = jnp.zeros((2, tokens, head_dim), F32)
        return carry

    lax.fori_loop(0, blocks, clear, 0)

    def bias_rows(i, carry):
        key = lax.broadcasted_iota(jnp.int32, (8, rows), 0) + i * 8 - core * tokens
        token = lax.broadcasted_iota(jnp.int32, (8, rows), 1) // heads
        bias[pl.ds(pl.multiple_of(i * 8, 8), 8)] = jnp.where(key <= token, 0.0, -jnp.inf)
        return carry

    lax.fori_loop(0, keys // 8, bias_rows, 0)
    own[0].wait()
    own[1].wait()

    def spread(f):
        for a in (1, 2):
            kv2(a, f).start()
        kvd(flip(f)).start()

    spread(0)

    def spread_rest(f, carry):
        kv1(f, 0).wait_recv()
        kv1(f, 1).wait_recv()
        spread(f)
        return carry

    lax.fori_loop(1, 4, spread_rest, 0)
    do_copy(1).start()
    do_copy(2).start()

    def wait_block(g):
        remote(kv.at[:, g], kv.at[:, g], kvd_s.at[g // 2], kv_r.at[g], sibling).wait_recv()

    def source(i):
        late = i // 8
        return (1 - late) * (1 + i % 2) + 3 * late, (1 - late) * (i // 2) + late * (i - 8)

    def arrive(i):
        a, f = source(i)
        g = member(a, f)
        wait_block(g)
        kvd(g).start()

        @pl.when(a + (f + f // 2) % 2 == 1)
        def _():
            kvf(g, f, 2).start()

        @pl.when((a - 1) * (2 - (f + f // 2) % 2) == 1)
        def _():
            kvf(g, f, 1).start()

    def use_chunk(g):
        wait_block(g + 1 - 2 * core)
        j = g // 2

        @pl.when(j < me // 2)
        def _():
            forward(0, j, False)

        @pl.when(j == me // 2)
        def _():
            forward(0, j, True)

    def gather_first(i, carry):
        arrive(i)
        use_chunk(flip(i))
        return carry

    def gather_next(i, carry):
        arrive(i)
        use_chunk(member(*source(i - 4)))
        return carry

    def gather_last(i, carry):
        use_chunk(member(*source(i)))
        return carry

    lax.fori_loop(0, 4, gather_first, 0)
    lax.fori_loop(4, 12, gather_next, 0)
    lax.fori_loop(8, 12, gather_last, 0)
    finish_slot(0)
    own_out[0].start()
    own_out[1].start()
    own[3].wait()
    prepare(0)

    def backward(f, j, masked):
        k_blk = load_chunk(0, j)
        v_blk = load_chunk(1, j)
        kt_blk = k_blk.T
        for r in range(rows // tile):
            cols = slice(r * tile, (r + 1) * tile)
            s = dot(k_blk, qt[f, :, cols]) * alpha
            if masked:
                s = s + bias[:, cols]
            p = jnp.exp2(s - lse2[f, :, cols])
            dp = dot(v_blk, dot_t[f, :, cols])
            ds = p * (dp - delta[f, :, cols])
            p_s[:, cols] = p.astype(BF16)
            ds_s[:, cols] = ds.astype(BF16)
        shape = (2, tokens, head_dim)
        dkdv[1, pl.ds(2 * j, 2)] += dot(p_s[...], dos[f]).reshape(shape)
        dkdv[0, pl.ds(2 * j, 2)] += dot(ds_s[...], qs[f]).reshape(shape)
        for r in range(rows // tile):
            cols = slice(r * tile, (r + 1) * tile)
            dqt[f, :, cols] += dot(kt_blk, ds_s[:, cols])

    def dq_copy(f):
        return remote(dq_st.at[f], dq_out.at[batch], dq_sem.at[0, f - 1], dq_sem.at[1, f - 1], flip(f))

    def finish_dq(f):
        for r in range(rows // tile):
            cols = slice(r * tile, (r + 1) * tile)
            dq_st[f, cols, :] = (dqt[f, :, cols] * scale).astype(BF16).T

    def middle_slot(f, carry):
        last = flip(f) // 2

        q_copy(f).wait_recv()

        @pl.when(f == 3)
        def _():
            q_copy(3).wait_send()
            do_copy(3).wait_send()
            pl.semaphore_signal(gate, inc=1, device_id={"cp": sibling}, device_id_type=pl.DeviceIdType.MESH)
            pl.semaphore_wait(gate, 1)
            for other in (2, 1):
                dq_copy(other).start()
            for other in (2, 1):
                o_copy(other).start()
                lse_copy(other).start()

        start_slot(f)

        def forward_body(j, inner):
            weigh(f, j, False, True)
            return inner

        scores_all(f, 0)
        lax.fori_loop(0, last, forward_body, 0)
        weigh(f, last, True, False)
        finish_slot(f)

        do_copy(f).wait_recv()

        @pl.when(f == 1)
        def _():
            do_copy(1).wait_send()
            do_copy(2).wait_send()
            q_copy(3).start()
            do_copy(3).start()

        prepare(f)

        @pl.when(f < 3)
        def _():
            def backward_body(j, inner):
                backward(f, j, False)
                return inner

            lax.fori_loop(0, last, backward_body, 0)
            backward(f, last, True)
            finish_dq(f)

        return carry

    lax.fori_loop(1, 4, middle_slot, 0)
    o_copy(3).start()
    lse_copy(3).start()

    def r1(j):
        return remote(dkdv.at[:, 2 * j + 1 - core], sib.at[:, j], r1_s.at[j], r1_r.at[j], sibling)

    def r2(g, a, f):
        i = (a - 1) * 4 + f
        return remote(dkdv.at[:, g], peer.at[i], r2_s.at[i], r2_r.at[i], group(a))

    def r2_relay(g, a, f):
        return remote(dkdv.at[:, g], relay.at[f], rl_s.at[f], rl_r.at[f], group(a))

    def order(t):
        stage, f = t // 4, t % 4
        first = (f + f // 2) % 2
        half, odd = stage // 2, stage % 2
        a = 3 * (1 - half) * (1 - odd) + (1 + first) * (1 - half) * odd + (2 - first) * half * (1 - odd)
        return member(a, f) // 2, a, f, first

    def reduce_pair(t):
        j, a, f, first = order(t)
        g = 2 * j + core
        r1(j).wait_recv()
        dkdv[:, g] += sib[:, j]

        @pl.when(t // 4 == 0)
        def _():
            r2_relay(g, 1 + first, f).start()

        @pl.when(t // 4 == 1)
        def _():
            r2(g, a, f).start()

    def second(f):
        a = 2 - (f + f // 2) % 2
        return r2(2 * (member(a, f) // 2) + core, a, f)

    def reduce_group(f):
        a = 2 - (f + f // 2) % 2
        g = 2 * (member(a, f) // 2) + core
        r2_relay(g, a, f).wait_recv()
        dkdv[:, g] += relay[f]
        second(f).start()

    def final_chunk(t, carry):
        j = order(t)[0]

        def slot(i, inner):
            f = 3 * i
            last = flip(f) // 2

            @pl.when(j < last)
            def _():
                backward(f, j, False)

            @pl.when(j == last)
            def _():
                backward(f, j, True)

            return inner

        lax.fori_loop(0, 2, slot, 0)
        r1(j).start()

        @pl.when(t > 0)
        def _():
            reduce_pair(t - 1)

        return carry

    lax.fori_loop(0, chunks, final_chunk, 0)
    finish_dq(3)
    dq_copy(3).start()
    finish_dq(0)
    own_out[2].start()
    reduce_pair(chunks - 1)
    reduce_group(3)
    reduce_group(1)
    second(3).wait_send()
    second(1).wait_send()
    reduce_group(0)
    reduce_group(2)

    def fin_copy(f, which):
        dst = (dk_out, dv_out)[which]
        return remote(fin.at[f, which], dst.at[batch], r3_s.at[which, f - 1], r3_r.at[which, f - 1], flip(f))

    def finish_kv(f):
        g = flip(f)
        for a in (1, 2):
            r2(g, a, f).wait_recv()
        total = dkdv[:, g] + peer[f] + peer[4 + f]
        fin[f, 0] = (total[0] * scale).astype(BF16)
        fin[f, 1] = total[1].astype(BF16)

    for f in (3, 1, 2, 0):
        finish_kv(f)
        if f:
            fin_copy(f, 0).start()
            fin_copy(f, 1).start()
        else:
            own_out[3].start()
            own_out[4].start()

    for f in (1, 2, 3):
        for which in (0, 1):
            kv1(f, which).wait_send()
            fin_copy(f, which).wait()
        if f < 3:
            q_copy(f).wait_send()
        o_copy(f).wait()
        lse_copy(f).wait()
        dq_copy(f).wait()
    for copy in own_out:
        copy.wait()

    def drain(i, carry):
        kv2(1 + i // 4, i % 4).wait_send()
        return carry

    lax.fori_loop(0, 8, drain, 0)
    for f in range(4):
        kvf(flip(f), f, 1).wait_send()
        r2(flip(f), 1 + (f + f // 2) % 2, f).wait_send()
        if f in (0, 2):
            second(f).wait_send()
        r2_relay(flip(f), 1, f).wait_send()

    def drain_sibling(j, carry):
        kvd(2 * j + core).wait_send()
        r1(j).wait_send()
        return carry

    lax.fori_loop(0, chunks, drain_sibling, 0)


def output_kernel(out_in, lse_in, dq_in, dk_in, dv_in, out, lse, dq, dk, dv, wide, narrow, rows_s, lse_s, sem_in, sem_out):
    batch, rows = lse_in.shape[0], lse_in.shape[2]
    heads, tokens = lse.shape[1], lse.shape[2]
    moves = []
    for i, (src, dst) in enumerate(((out_in, out), (dq_in, dq))):
        for b in range(batch):
            moves.append((src.at[b], wide.at[i, b], dst.at[b]))
    for i, (src, dst) in enumerate(((dk_in, dk), (dv_in, dv))):
        moves.append((src, narrow.at[i], dst))
    steps = [(pltpu.make_async_copy(src, mid, sem_in.at[i]), pltpu.make_async_copy(mid, dst, sem_out.at[i]))
             for i, (src, mid, dst) in enumerate(moves)]
    last = len(steps)
    lse_load = pltpu.make_async_copy(lse_in, rows_s, sem_in.at[last])
    lse_store = pltpu.make_async_copy(lse_s, lse, sem_out.at[last])
    lse_load.start()
    for load, _ in steps:
        load.start()
    lse_load.wait()
    head = lax.broadcasted_iota(jnp.int32, (heads, rows), 0)
    mine = lax.broadcasted_iota(jnp.int32, (heads, rows), 1) % heads == head
    token = lax.broadcasted_iota(jnp.int32, (rows, tokens), 1)
    pick = jnp.where(lax.broadcasted_iota(jnp.int32, (rows, tokens), 0) // heads == token, 1.0, 0.0).astype(BF16)
    rest = jnp.concatenate([jnp.where(mine, rows_s[b], 0.0) for b in range(batch)], axis=0)
    total = jnp.zeros((batch * heads, tokens), F32)
    for _ in range(3):
        part = rest.astype(BF16)
        total = total + dot(part, pick)
        rest = rest - part.astype(F32)
    lse_s[...] = total.reshape(batch, heads, tokens)
    for i, (load, store) in enumerate(steps):
        load.wait()
        store.start()
        if i == 3:
            lse_store.start()
    lse_store.wait()
    for _, store in steps:
        store.wait()


def solution(mesh):
    cp_size = mesh.shape["cp"]

    def attention_shard(queries, keys, values, out_grad):
        batch, tokens, heads, head_dim = queries.shape
        rows = tokens * heads
        q_rows = queries.reshape(batch, rows, head_dim)
        do_rows = out_grad.reshape(batch, rows, head_dim)
        k_rows = keys.reshape(batch, tokens, head_dim)
        v_rows = values.reshape(batch, tokens, head_dim)
        any_spec = pl.BlockSpec(memory_space=pl.ANY)
        dma = pltpu.SemaphoreType.DMA
        block = (tokens, head_dim)
        shapes = [
            jax.ShapeDtypeStruct((batch, rows, head_dim), BF16),
            jax.ShapeDtypeStruct((batch, 1, rows), F32),
            jax.ShapeDtypeStruct((batch, rows, head_dim), BF16),
            jax.ShapeDtypeStruct((batch,) + block, BF16),
            jax.ShapeDtypeStruct((batch,) + block, BF16),
        ]
        scratch = [
            pltpu.VMEM((4, rows, head_dim), BF16),
            pltpu.VMEM((4, rows, head_dim), BF16),
            pltpu.VMEM((4, head_dim, rows), BF16),
            pltpu.VMEM((4, head_dim, rows), BF16),
            pltpu.VMEM((2, cp_size) + block, BF16),
            pltpu.VMEM((head_dim, rows), F32),
            pltpu.VMEM((4, head_dim, rows), BF16),
            pltpu.VMEM((4, rows, head_dim), BF16),
            pltpu.VMEM((1, rows), F32),
            pltpu.VMEM((8, rows), F32),
            pltpu.VMEM((4, 1, rows), F32),
            pltpu.VMEM((4, 1, rows), F32),
            pltpu.VMEM((4, 1, rows), F32),
            pltpu.VMEM((2 * tokens, rows), F32),
            pltpu.VMEM((2 * tokens, rows), F32),
            pltpu.VMEM((8, rows), F32),
            pltpu.VMEM((2 * tokens, rows), BF16),
            pltpu.VMEM((2 * tokens, rows), BF16),
            pltpu.VMEM((4, head_dim, rows), F32),
            pltpu.VMEM((4, rows, head_dim), BF16),
            pltpu.VMEM((2, cp_size) + block, F32),
            pltpu.VMEM((2, cp_size // 2) + block, F32),
            pltpu.VMEM((8, 2) + block, F32),
            pltpu.VMEM((4, 2) + block, F32),
            pltpu.VMEM((4, 2) + block, BF16),
            dma((9,)), dma((2, 3)), dma((2, 3)), dma((8,)), dma((4,)), dma((cp_size // 2,)), dma((cp_size,)),
            dma((2, 3)), dma((2, 3)), dma((2, 3)), dma((2, 3)), dma((2, 3)),
            dma((cp_size // 2,)), dma((cp_size // 2,)), dma((8,)), dma((8,)), dma((4,)), dma((4,)), dma((2, 3)), dma((2, 3)),
            pltpu.SemaphoreType.REGULAR,
        ]
        out, lse, dq, dk, dv = pl.pallas_call(
            attention_kernel,
            out_shape=shapes,
            in_specs=[any_spec] * 4,
            out_specs=[any_spec] * 5,
            scratch_shapes=scratch,
            name="attention",
            compiler_params=pltpu.CompilerParams(
                collective_id=0, has_side_effects=True, vmem_limit_bytes=60 * 1024 * 1024),
        )(q_rows, do_rows, k_rows, v_rows)
        out, row_lse, dq, dk, dv = pl.pallas_call(
            output_kernel,
            out_shape=[shapes[0], jax.ShapeDtypeStruct((batch, heads, tokens), F32)] + shapes[2:],
            in_specs=[any_spec] * 5,
            out_specs=[any_spec] * 5,
            scratch_shapes=[
                pltpu.VMEM((2, batch, rows, head_dim), BF16), pltpu.VMEM((2, batch) + block, BF16),
                pltpu.VMEM((batch, 1, rows), F32), pltpu.VMEM((batch, heads, tokens), F32),
                dma((2 * batch + 3,)), dma((2 * batch + 3,))],
            name="outputs",
            compiler_params=pltpu.CompilerParams(vmem_limit_bytes=60 * 1024 * 1024),
        )(out, lse, dq, dk, dv)
        return out.reshape(queries.shape), row_lse, dq.reshape(queries.shape), dk.reshape(keys.shape), dv.reshape(values.shape)

    seq_spec = P("dp", "cp")
    return jax.shard_map(attention_shard, mesh=mesh, in_specs=(seq_spec, seq_spec, seq_spec, seq_spec), out_specs=(seq_spec, P("dp", None, "cp"), seq_spec, seq_spec, seq_spec), check_vma=False)
```
